16 devices in a mesh: dp: 2 (over z), tp: 8 (over y, x, core).
Axes of the slice: x: 2, y: 2, z: 2, core: 2. Of those that a mesh axis runs over, the one named last changes fastest.
Arguments:
- x_in: bfloat16 [256, 4096], P('dp'), parts along dimension 0
- tok_pos: int32 [256], P('dp'), parts along dimension 0
- self_k: bfloat16 [256, 64, 64, 64], P('dp', None, 'tp'), parts along dimension 0
- self_v: bfloat16 [256, 64, 64, 64], P('dp', None, 'tp'), parts along dimension 0
- cross_k: bfloat16 [256, 128, 64, 64], P('dp', None, 'tp'), parts along dimension 0
- cross_v: bfloat16 [256, 128, 64, 64], P('dp', None, 'tp'), parts along dimension 0
- enc_mask: int32 [256, 128], P('dp'), parts along dimension 0
- rel_bias: float32 [32, 64], P(None, 'tp')
- w_q: bfloat16 [4096, 4096], P(None, 'tp')
- w_k: bfloat16 [4096, 4096], P(None, 'tp')
- w_v: bfloat16 [4096, 4096], P(None, 'tp')
- w_o: bfloat16 [4096, 4096], P('tp')
- cross_q: bfloat16 [4096, 4096], P(None, 'tp')
- cross_o: bfloat16 [4096, 4096], P('tp')
- w_gate: bfloat16 [4096, 10240], P(None, 'tp')
- w_up: bfloat16 [4096, 10240], P(None, 'tp')
- w_down: bfloat16 [10240, 4096], P('tp')
- norm_self: bfloat16 [4096], replicated
- norm_cross: bfloat16 [4096], replicated
- norm_mlp: bfloat16 [4096], replicated
Outputs:
- output 1: bfloat16 [256, 4096], P('dp'), parts along dimension 0
- output 2: bfloat16 [256, 64, 64, 64], P('dp', None, 'tp'), parts along dimension 0
- output 3: bfloat16 [256, 64, 64, 64], P('dp', None, 'tp'), parts along dimension 0
There are 2 independent parts. The reference program is written for one: setup_inputs(seed, part) draws one part's arguments, and reference() takes and returns one part's arrays. A program takes and returns all parts, laid end to end along the dimension named above; an argument that names none is the same for every part.
All inputs are finite; a program needn't handle non-finite values.
Results may differ from the reference program's by a relative error of at most 0.0192555.
Values are sent between devices in bfloat16 or wider.
A program may use at most 1 GiB of HBM per device.

```python
import math
import jax
import jax.numpy as jnp
from jax import lax

BATCH_ROWS = 128
T_MAX = 64
SRC_LEN = 128
D_MODEL = 4096
N_HEADS = 64
D_HEAD = 64
D_FF = 10240

INNER_DIM = N_HEADS * D_HEAD
BUCKET_EDGES = tuple(int(math.ceil(16.0 * 8.0 ** (bucket_step / 16.0))) for bucket_step in range(1, 16))
NEG_FILL = -1e30


def draw_ends(rng_key, low_end, high_end):
    key_list = jax.random.split(rng_key, 3)
    drawn_vals = jax.random.randint(key_list[0], (BATCH_ROWS,), low_end, high_end + 1)
    high_row = jax.random.randint(key_list[1], (), 0, BATCH_ROWS)
    low_row = (high_row + jax.random.randint(key_list[2], (), 1, BATCH_ROWS)) % BATCH_ROWS
    return drawn_vals.at[high_row].set(high_end).at[low_row].set(low_end).astype(jnp.int32)


def normal_bf16(rng_key, array_shape, std_dev):
    return (std_dev * jax.random.normal(rng_key, array_shape, jnp.float32)).astype(jnp.bfloat16)


def setup_inputs(seed: int = 0, part: int = 0) -> dict:
    part_keys = jax.random.split(jax.random.fold_in(jax.random.key(seed), part), 8)
    shared_keys = jax.random.split(jax.random.key(seed + 1), 16)
    cache_shape = (BATCH_ROWS, T_MAX, N_HEADS, D_HEAD)
    cross_shape = (BATCH_ROWS, SRC_LEN, N_HEADS, D_HEAD)
    src_lens = draw_ends(part_keys[2], SRC_LEN // 4, SRC_LEN)
    bias_draw = 0.7 * jax.random.normal(shared_keys[0], (32, N_HEADS), jnp.float32)
    q_scale = (D_MODEL * D_HEAD) ** -0.5
    in_scale = D_MODEL ** -0.5
    out_scale = INNER_DIM ** -0.5
    return {
        'x_in': normal_bf16(part_keys[0], (BATCH_ROWS, D_MODEL), 1.0),
        'tok_pos': draw_ends(part_keys[1], T_MAX // 8, T_MAX - 1),
        'self_k': normal_bf16(part_keys[3], cache_shape, 1.0),
        'self_v': normal_bf16(part_keys[4], cache_shape, 1.0),
        'cross_k': normal_bf16(part_keys[5], cross_shape, 1.0),
        'cross_v': normal_bf16(part_keys[6], cross_shape, 1.0),
        'enc_mask': (jnp.arange(SRC_LEN)[None, :] < src_lens[:, None]).astype(jnp.int32),
        'rel_bias': bias_draw.at[0].add(0.5 * math.log(T_MAX) - 1.0),
        'w_q': normal_bf16(shared_keys[1], (D_MODEL, INNER_DIM), q_scale),
        'w_k': normal_bf16(shared_keys[2], (D_MODEL, INNER_DIM), in_scale),
        'w_v': normal_bf16(shared_keys[3], (D_MODEL, INNER_DIM), in_scale),
        'w_o': normal_bf16(shared_keys[4], (INNER_DIM, D_MODEL), 0.4 * math.sqrt(T_MAX) * out_scale),
        'cross_q': normal_bf16(shared_keys[5], (D_MODEL, INNER_DIM), q_scale),
        'cross_o': normal_bf16(shared_keys[6], (INNER_DIM, D_MODEL), 0.5 * math.sqrt(SRC_LEN) * out_scale),
        'w_gate': normal_bf16(shared_keys[7], (D_MODEL, D_FF), in_scale),
        'w_up': normal_bf16(shared_keys[8], (D_MODEL, D_FF), in_scale),
        'w_down': normal_bf16(shared_keys[9], (D_FF, D_MODEL), 1.5 * D_FF ** -0.5),
        'norm_self': (1.0 + 0.25 * jax.random.normal(shared_keys[10], (D_MODEL,), jnp.float32)).astype(jnp.bfloat16),
        'norm_cross': (1.0 + 0.25 * jax.random.normal(shared_keys[11], (D_MODEL,), jnp.float32)).astype(jnp.bfloat16),
        'norm_mlp': (1.0 + 0.25 * jax.random.normal(shared_keys[12], (D_MODEL,), jnp.float32)).astype(jnp.bfloat16),
    }


def rms_norm(values, norm_scale):
    inv_rms = lax.rsqrt(jnp.mean(values * values, axis=-1, keepdims=True) + 1e-6)
    return (values * inv_rms * norm_scale.astype(jnp.float32)).astype(jnp.bfloat16)


def project(normed, weight):
    return jnp.dot(normed, weight, preferred_element_type=jnp.float32).astype(jnp.bfloat16)


def rel_bucket(distance):
    bucket_edges = jnp.array(BUCKET_EDGES, dtype=jnp.int32)
    far_bucket = 16 + jnp.sum((distance[..., None] >= bucket_edges).astype(jnp.int32), axis=-1)
    return jnp.where(distance < 16, distance, far_bucket)


def attend(queries, keys_all, values_all, extra):
    def one_row(operands):
        row_q, row_k, row_v, row_extra = operands
        scores = jnp.einsum('hk,thk->ht', row_q.astype(jnp.float32), row_k.astype(jnp.float32)) + row_extra
        probs_bf = jax.nn.softmax(scores, axis=-1).astype(jnp.bfloat16)
        mixed_out = jnp.einsum('ht,thk->hk', probs_bf.astype(jnp.float32), row_v.astype(jnp.float32))
        return mixed_out.astype(jnp.bfloat16)
    return lax.map(one_row, (queries, keys_all, values_all, extra))


def reference(x_in, tok_pos, self_k, self_v, cross_k, cross_v, enc_mask, rel_bias, w_q, w_k, w_v, w_o, cross_q, cross_o, w_gate, w_up, w_down, norm_self, norm_cross, norm_mlp):
    row_count = x_in.shape[0]
    head_shape = (row_count, N_HEADS, D_HEAD)
    residual = x_in.astype(jnp.float32)
    normed = rms_norm(residual, norm_self)
    queries = project(normed, w_q).reshape(head_shape)
    new_keys = project(normed, w_k).reshape(head_shape)
    new_values = project(normed, w_v).reshape(head_shape)
    key_index = jnp.arange(T_MAX)
    at_pos = (key_index[None, :] == tok_pos[:, None])[:, :, None, None]
    new_self_k = jnp.where(at_pos, new_keys[:, None], self_k)
    new_self_v = jnp.where(at_pos, new_values[:, None], self_v)
    distance = jnp.maximum(tok_pos[:, None] - key_index[None, :], 0)
    bias_rows = jnp.swapaxes(jnp.take(rel_bias, rel_bucket(distance), axis=0), 1, 2)
    causal = (key_index[None, :] <= tok_pos[:, None])[:, None, :]
    self_extra = jnp.where(causal, bias_rows, NEG_FILL)
    mixed_self = attend(queries, new_self_k, new_self_v, self_extra)
    residual = residual + jnp.dot(mixed_self.reshape(row_count, INNER_DIM), w_o, preferred_element_type=jnp.float32)
    normed = rms_norm(residual, norm_cross)
    cross_queries = project(normed, cross_q).reshape(head_shape)
    cross_extra = jnp.where(enc_mask[:, None, :] != 0, 0.0, NEG_FILL)
    mixed_cross = attend(cross_queries, cross_k, cross_v, cross_extra)
    residual = residual + jnp.dot(mixed_cross.reshape(row_count, INNER_DIM), cross_o, preferred_element_type=jnp.float32)
    normed = rms_norm(residual, norm_mlp)
    gate_pre = jnp.dot(normed, w_gate, preferred_element_type=jnp.float32)
    up_pre = jnp.dot(normed, w_up, preferred_element_type=jnp.float32)
    hidden = (jax.nn.gelu(gate_pre, approximate=True) * up_pre).astype(jnp.bfloat16)
    residual = residual + jnp.dot(hidden, w_down, preferred_element_type=jnp.float32)
    return (residual.astype(jnp.bfloat16), new_self_k, new_self_v)
```

```python
import math
import jax
import jax.numpy as jnp
import numpy as np
from jax import lax
from jax.experimental import pallas as pl
from jax.experimental.pallas import tpu as pltpu
from jax.sharding import PartitionSpec as P

F32 = jnp.float32
BF16 = jnp.bfloat16
BUCKET_EDGES = tuple(int(math.ceil(16.0 * 8.0 ** (bucket_step / 16.0))) for bucket_step in range(1, 16))
NEG_FILL = -1e30
ROWS, T_LEN, S_LEN, HEADS, HEAD_DIM = 128, 64, 128, 8, 64
D_MODEL, FLAT, UNITS = 4096, 512, 1280
K_CHUNK = 1024
N_CHUNK = D_MODEL // K_CHUNK


def rms_norm(values, norm_scale):
    inv_rms = lax.rsqrt(jnp.mean(values * values, axis=-1, keepdims=True) + 1e-6)
    return (values * inv_rms * norm_scale).astype(BF16)


def bias_table(rel_bias_t, tok_row):
    step = lax.broadcasted_iota(jnp.int32, (T_LEN, 32), 0)
    bucket = lax.broadcasted_iota(jnp.int32, (T_LEN, 32), 1)
    distance = (T_LEN - 1) - step
    far = jnp.full_like(distance, 16)
    for edge in BUCKET_EDGES:
        far = far + (distance >= edge).astype(jnp.int32)
    own_bucket = jnp.where(distance < 16, distance, far)
    one_hot = (bucket == own_bucket).astype(F32)
    by_step = lax.dot_general(one_hot, rel_bias_t, (((1,), (1,)), ((), ())),
                              precision=lax.Precision.HIGHEST, preferred_element_type=F32)
    shift = (T_LEN - 1) - tok_row
    position = lax.broadcasted_iota(jnp.int32, (T_LEN, ROWS), 0)
    allowed = position <= tok_row
    tables = []
    for head in range(HEADS):
        table = jnp.broadcast_to(by_step[:, head:head + 1], (T_LEN, ROWS))
        for bit in (32, 16, 8, 4, 2, 1):
            moved = jnp.concatenate([table[bit:], table[:bit]], axis=0)
            table = jnp.where((shift & bit) != 0, moved, table)
        tables.append(jnp.where(allowed, table, NEG_FILL))
    return tables


def self_kernel(x_hbm, tok_ref, rel_ref, norm_ref, wq, wk, wv, wo, sk, sv,
                part_ref, nk, nv,
                x_buf, h_buf, w_buf, wo_buf, k_buf, v_buf, acc, q_t, kn_t, vn_t, bias, probs, mix,
                x_sem, w_sem, wo_sem, k_sem, v_sem, ko_sem, vo_sem):
    x_copy = pltpu.make_async_copy(x_hbm, x_buf, x_sem)
    x_copy.start()
    srcs = (wq, wk, wv)

    def w_copy(chunk, which):
        rows = pl.ds(pl.multiple_of(chunk * K_CHUNK, K_CHUNK), K_CHUNK)
        return pltpu.make_async_copy(srcs[which].at[rows, :], w_buf.at[rows, pl.ds(which * FLAT, FLAT)],
                                     w_sem.at[chunk, which])

    def in_copy(src, buf, sem, head):
        return pltpu.make_async_copy(src.at[:, head], buf.at[head], sem.at[head])

    def out_copy(buf, dst, sem, head):
        return pltpu.make_async_copy(buf.at[head], dst.at[:, head], sem.at[head])

    for chunk in range(N_CHUNK):
        for which in range(3):
            w_copy(chunk, which).start()

    def start_in(head, carry):
        in_copy(sk, k_buf, k_sem, head).start()
        in_copy(sv, v_buf, v_sem, head).start()
        return carry
    lax.fori_loop(0, HEADS, start_in, 0)
    wo_copy = pltpu.make_async_copy(wo, wo_buf, wo_sem)
    wo_copy.start()

    tok_row = tok_ref[...]
    for head, table in enumerate(bias_table(rel_ref[...], tok_row)):
        bias[head] = table

    x_copy.wait()

    def norm_rows(step, carry):
        rows = pl.ds(pl.multiple_of(step * 16, 16), 16)
        h_buf[rows, :] = rms_norm(x_buf[rows, :].astype(F32), norm_ref[...].astype(F32))
        return carry
    lax.fori_loop(0, ROWS // 16, norm_rows, 0)

    acc[...] = jnp.zeros_like(acc)

    def qkv_step(chunk, carry):
        for which in range(3):
            w_copy(chunk, which).wait()
            rows = pl.ds(pl.multiple_of(chunk * K_CHUNK, K_CHUNK), K_CHUNK)
            cols = slice(which * FLAT, (which + 1) * FLAT)
            acc[:, cols] += jnp.dot(h_buf[:, rows], w_buf[rows, cols], preferred_element_type=F32)
        return carry
    lax.fori_loop(0, N_CHUNK, qkv_step, 0)

    for which, dst in enumerate((q_t, kn_t, vn_t)):
        for block in range(FLAT // 128):
            start = which * FLAT + block * 128
            turned = jnp.transpose(acc[:, start:start + 128])
            dst[block * 128:(block + 1) * 128, :] = turned.astype(BF16).astype(dst.dtype)

    tok_b = jnp.broadcast_to(tok_row.astype(F32), (HEAD_DIM, ROWS)).astype(BF16)

    def head_step(head, carry):
        lanes = pl.ds(pl.multiple_of(head * HEAD_DIM, HEAD_DIM), HEAD_DIM)
        in_copy(sk, k_buf, k_sem, head).wait()
        query = q_t[lanes, :]
        fresh_k = kn_t[lanes, :]

        def score_group(group, inner):
            at_tok = tok_b - (group * 8).astype(F32).astype(BF16)
            rows = []
            for i in range(8):
                step = group * 8 + i
                keys = jnp.where(at_tok == jnp.asarray(i, BF16), fresh_k, k_buf[head, step])
                k_buf[head, step] = keys
                rows.append(jnp.sum(keys.astype(F32) * query, axis=0, keepdims=True))
            probs[pl.ds(pl.multiple_of(group * 8, 8), 8), :] = jnp.concatenate(rows, axis=0)
            return inner
        lax.fori_loop(0, T_LEN // 8, score_group, 0)
        out_copy(k_buf, nk, ko_sem, head).start()
        scores = probs[...] + bias[head]
        weights = jnp.exp(scores - jnp.max(scores, axis=0, keepdims=True))
        weights = weights / jnp.sum(weights, axis=0, keepdims=True)
        probs[...] = weights.astype(BF16).astype(F32)
        in_copy(sv, v_buf, v_sem, head).wait()
        fresh_v = vn_t[lanes, :]

        def mix_group(group, total):
            at_tok = tok_b - (group * 8).astype(F32).astype(BF16)
            for i in range(8):
                step = group * 8 + i
                vals = jnp.where(at_tok == jnp.asarray(i, BF16), fresh_v, v_buf[head, step])
                v_buf[head, step] = vals
                total = total + vals.astype(F32) * probs[pl.ds(step, 1), :]
            return total
        mix[lanes, :] = lax.fori_loop(0, T_LEN // 8, mix_group, jnp.zeros((HEAD_DIM, ROWS), F32))
        out_copy(v_buf, nv, vo_sem, head).start()
        return carry
    lax.fori_loop(0, HEADS, head_step, 0)

    mixed = jnp.concatenate([jnp.transpose(mix[block * 128:(block + 1) * 128, :]).astype(BF16)
                             for block in range(FLAT // 128)], axis=1)
    wo_copy.wait()

    def o_step(block, carry):
        cols = pl.ds(pl.multiple_of(block * 512, 512), 512)
        part_ref[:, cols] = jnp.dot(mixed, wo_buf[:, cols], preferred_element_type=F32).astype(BF16)
        return carry
    lax.fori_loop(0, D_MODEL // 512, o_step, 0)

    def end_out(head, carry):
        out_copy(k_buf, nk, ko_sem, head).wait()
        out_copy(v_buf, nv, vo_sem, head).wait()
        return carry
    lax.fori_loop(0, HEADS, end_out, 0)


def self_stage(x_in, tok_row, rel_t, norm_row, w_q, w_k, w_v, w_o, sk_t, sv_t):
    hbm = pl.BlockSpec(memory_space=pl.ANY)
    vmem = pl.BlockSpec(memory_space=pltpu.VMEM)
    cache = jax.ShapeDtypeStruct((T_LEN, HEADS, HEAD_DIM, ROWS), BF16)
    dma = pltpu.SemaphoreType.DMA
    return pl.pallas_call(
        self_kernel,
        out_shape=(jax.ShapeDtypeStruct((ROWS, D_MODEL), BF16), cache, cache),
        in_specs=[hbm, vmem, vmem, vmem] + [hbm] * 6,
        out_specs=(vmem, hbm, hbm),
        scratch_shapes=[
            pltpu.VMEM((ROWS, D_MODEL), BF16), pltpu.VMEM((ROWS, D_MODEL), BF16),
            pltpu.VMEM((D_MODEL, 3 * FLAT), BF16), pltpu.VMEM((FLAT, D_MODEL), BF16),
            pltpu.VMEM((HEADS, T_LEN, HEAD_DIM, ROWS), BF16), pltpu.VMEM((HEADS, T_LEN, HEAD_DIM, ROWS), BF16),
            pltpu.VMEM((ROWS, 3 * FLAT), F32), pltpu.VMEM((FLAT, ROWS), F32),
            pltpu.VMEM((FLAT, ROWS), BF16), pltpu.VMEM((FLAT, ROWS), BF16),
            pltpu.VMEM((HEADS, T_LEN, ROWS), F32), pltpu.VMEM((T_LEN, ROWS), F32), pltpu.VMEM((FLAT, ROWS), F32),
            dma, dma((N_CHUNK, 3)), dma, dma((HEADS,)), dma((HEADS,)), dma((HEADS,)), dma((HEADS,)),
        ],
        compiler_params=pltpu.CompilerParams(vmem_limit_bytes=56 * 1024 * 1024),
        cost_estimate=pl.CostEstimate(flops=10 ** 9, bytes_accessed=50 * 2 ** 20, transcendentals=0),
        name='self_stage',
    )(x_in, tok_row, rel_t, norm_row, w_q, w_k, w_v, w_o, sk_t, sv_t)


def project(normed, weight):
    return jnp.dot(normed, weight, preferred_element_type=F32).astype(BF16)


def attend(queries, keys_all, values_all, extra):
    scores = jnp.einsum('bhk,bthk->bht', queries, keys_all, preferred_element_type=jnp.float32) + extra
    probs_bf = jax.nn.softmax(scores, axis=-1).astype(jnp.bfloat16)
    mixed_out = jnp.einsum('bht,bthk->bhk', probs_bf, values_all, preferred_element_type=jnp.float32)
    return mixed_out.astype(jnp.bfloat16)


def solution(mesh):
    def tp_sum(partial_out):
        return lax.psum(partial_out.astype(jnp.bfloat16), 'tp').astype(jnp.float32)

    def local_layer(x_in, tok_pos, self_k, self_v, cross_k, cross_v, enc_mask, rel_bias, w_q, w_k, w_v, w_o, cross_q, cross_o, w_gate, w_up, w_down, norm_self, norm_cross, norm_mlp):
        head_shape = (ROWS, HEADS, HEAD_DIM)
        part, new_k, new_v = self_stage(
            x_in, tok_pos.reshape(1, ROWS), rel_bias.T, norm_self.reshape(1, D_MODEL), w_q, w_k, w_v, w_o,
            jnp.transpose(self_k, (1, 2, 3, 0)), jnp.transpose(self_v, (1, 2, 3, 0)))
        new_self_k = jnp.transpose(new_k, (3, 0, 1, 2))
        new_self_v = jnp.transpose(new_v, (3, 0, 1, 2))
        residual = x_in.astype(F32) + tp_sum(part)
        normed = rms_norm(residual, norm_cross.astype(F32))
        cross_queries = project(normed, cross_q).reshape(head_shape)
        cross_extra = jnp.where(enc_mask[:, None, :] != 0, 0.0, NEG_FILL)
        mixed_cross = attend(cross_queries, cross_k, cross_v, cross_extra)
        residual = residual + tp_sum(jnp.dot(mixed_cross.reshape(ROWS, FLAT), cross_o, preferred_element_type=jnp.float32))
        normed = rms_norm(residual, norm_mlp.astype(F32))
        gate_pre = jnp.dot(normed, w_gate, preferred_element_type=jnp.float32)
        up_pre = jnp.dot(normed, w_up, preferred_element_type=jnp.float32)
        hidden = (jax.nn.gelu(gate_pre, approximate=True) * up_pre).astype(jnp.bfloat16)
        residual = residual + tp_sum(jnp.dot(hidden, w_down, preferred_element_type=jnp.float32))
        return residual.astype(jnp.bfloat16), new_self_k, new_self_v

    cache_spec = P('dp', None, 'tp', None)
    split_cols = P(None, 'tp')
    split_rows = P('tp', None)
    in_specs = (P('dp', None), P('dp'), cache_spec, cache_spec, cache_spec, cache_spec, P('dp', None), P(None, 'tp'), split_cols, split_cols, split_cols, split_rows, split_cols, split_rows, split_cols, split_cols, split_rows, P(None), P(None), P(None))
    out_specs = (P('dp', None), cache_spec, cache_spec)
    return jax.shard_map(local_layer, mesh=mesh, in_specs=in_specs, out_specs=out_specs, check_vma=False)
```

```python
import math
import jax
import jax.numpy as jnp
import numpy as np
from jax import lax
from jax.experimental import pallas as pl
from jax.experimental.pallas import tpu as pltpu
from jax.sharding import PartitionSpec as P

F32 = jnp.float32
BF16 = jnp.bfloat16
BUCKET_EDGES = tuple(int(math.ceil(16.0 * 8.0 ** (bucket_step / 16.0))) for bucket_step in range(1, 16))
NEG_FILL = -1e30
ROWS, T_LEN, S_LEN, HEADS, HEAD_DIM = 128, 64, 128, 8, 64
D_MODEL, FLAT, UNITS = 4096, 512, 1280
K_CHUNK = 1024
N_CHUNK = D_MODEL // K_CHUNK


def rms_norm(values, norm_scale):
    inv_rms = lax.rsqrt(jnp.mean(values * values, axis=-1, keepdims=True) + 1e-6)
    return (values * inv_rms * norm_scale).astype(BF16)


def bias_table(rel_bias_t, tok_row):
    step = lax.broadcasted_iota(jnp.int32, (T_LEN, 32), 0)
    bucket = lax.broadcasted_iota(jnp.int32, (T_LEN, 32), 1)
    distance = (T_LEN - 1) - step
    far = jnp.full_like(distance, 16)
    for edge in BUCKET_EDGES:
        far = far + (distance >= edge).astype(jnp.int32)
    own_bucket = jnp.where(distance < 16, distance, far)
    one_hot = (bucket == own_bucket).astype(F32)
    by_step = lax.dot_general(one_hot, rel_bias_t, (((1,), (1,)), ((), ())),
                              precision=lax.Precision.HIGHEST, preferred_element_type=F32)
    shift = (T_LEN - 1) - tok_row
    position = lax.broadcasted_iota(jnp.int32, (T_LEN, ROWS), 0)
    allowed = position <= tok_row
    tables = []
    for head in range(HEADS):
        table = jnp.broadcast_to(by_step[:, head:head + 1], (T_LEN, ROWS))
        for bit in (32, 16, 8, 4, 2, 1):
            moved = jnp.concatenate([table[bit:], table[:bit]], axis=0)
            table = jnp.where((shift & bit) != 0, moved, table)
        tables.append(jnp.where(allowed, table, NEG_FILL))
    return tables


def self_kernel(x_hbm, tok_ref, rel_ref, norm_ref, wq, wk, wv, wo, sk, sv,
                part_ref, nk, nv,
                x_buf, h_buf, w_buf, wo_buf, k_buf, v_buf, acc, q_t, kn_t, vn_t, bias, probs, mix,
                x_sem, w_sem, wo_sem, k_sem, v_sem, ko_sem, vo_sem):
    x_copy = pltpu.make_async_copy(x_hbm, x_buf, x_sem)
    x_copy.start()
    srcs = (wq, wk, wv)

    def w_copy(chunk, which):
        rows = pl.ds(pl.multiple_of(chunk * K_CHUNK, K_CHUNK), K_CHUNK)
        return pltpu.make_async_copy(srcs[which].at[rows, :], w_buf.at[rows, pl.ds(which * FLAT, FLAT)],
                                     w_sem.at[chunk, which])

    def in_copy(src, buf, sem, head):
        return pltpu.make_async_copy(src.at[:, head], buf.at[head], sem.at[head])

    def out_copy(buf, dst, sem, head):
        return pltpu.make_async_copy(buf.at[head], dst.at[:, head], sem.at[head])

    for chunk in range(N_CHUNK):
        for which in range(3):
            w_copy(chunk, which).start()

    def start_in(head, carry):
        in_copy(sk, k_buf, k_sem, head).start()
        in_copy(sv, v_buf, v_sem, head).start()
        return carry
    lax.fori_loop(0, HEADS, start_in, 0)
    wo_copy = pltpu.make_async_copy(wo, wo_buf, wo_sem)
    wo_copy.start()

    tok_row = tok_ref[...]
    for head, table in enumerate(bias_table(rel_ref[...], tok_row)):
        bias[head] = table

    x_copy.wait()

    def norm_rows(step, carry):
        rows = pl.ds(pl.multiple_of(step * 16, 16), 16)
        h_buf[rows, :] = rms_norm(x_buf[rows, :].astype(F32), norm_ref[...].astype(F32))
        return carry
    lax.fori_loop(0, ROWS // 16, norm_rows, 0)

    acc[...] = jnp.zeros_like(acc)

    def qkv_step(chunk, carry):
        for which in range(3):
            w_copy(chunk, which).wait()
            rows = pl.ds(pl.multiple_of(chunk * K_CHUNK, K_CHUNK), K_CHUNK)
            cols = slice(which * FLAT, (which + 1) * FLAT)
            acc[:, cols] += jnp.dot(h_buf[:, rows], w_buf[rows, cols], preferred_element_type=F32)
        return carry
    lax.fori_loop(0, N_CHUNK, qkv_step, 0)

    for which, dst in enumerate((q_t, kn_t, vn_t)):
        for block in range(FLAT // 128):
            start = which * FLAT + block * 128
            turned = jnp.transpose(acc[:, start:start + 128])
            dst[block * 128:(block + 1) * 128, :] = turned.astype(BF16).astype(dst.dtype)

    tok_b = jnp.broadcast_to(tok_row.astype(F32), (HEAD_DIM, ROWS)).astype(BF16)

    def head_step(head, carry):
        lanes = pl.ds(pl.multiple_of(head * HEAD_DIM, HEAD_DIM), HEAD_DIM)
        in_copy(sk, k_buf, k_sem, head).wait()
        query = q_t[lanes, :]
        fresh_k = kn_t[lanes, :]

        def score_group(group, inner):
            at_tok = tok_b - (group * 8).astype(F32).astype(BF16)
            rows = []
            for i in range(8):
                step = group * 8 + i
                keys = jnp.where(at_tok == jnp.asarray(i, BF16), fresh_k, k_buf[head, step])
                k_buf[head, step] = keys
                rows.append(jnp.sum(keys.astype(F32) * query, axis=0, keepdims=True))
            probs[pl.ds(pl.multiple_of(group * 8, 8), 8), :] = jnp.concatenate(rows, axis=0)
            return inner
        lax.fori_loop(0, T_LEN // 8, score_group, 0)
        out_copy(k_buf, nk, ko_sem, head).start()
        scores = probs[...] + bias[head]
        weights = jnp.exp(scores - jnp.max(scores, axis=0, keepdims=True))
        weights = weights / jnp.sum(weights, axis=0, keepdims=True)
        probs[...] = weights.astype(BF16).astype(F32)
        in_copy(sv, v_buf, v_sem, head).wait()
        fresh_v = vn_t[lanes, :]

        def mix_group(group, total):
            at_tok = tok_b - (group * 8).astype(F32).astype(BF16)
            for i in range(8):
                step = group * 8 + i
                vals = jnp.where(at_tok == jnp.asarray(i, BF16), fresh_v, v_buf[head, step])
                v_buf[head, step] = vals
                total = total + vals.astype(F32) * probs[pl.ds(step, 1), :]
            return total
        mix[lanes, :] = lax.fori_loop(0, T_LEN // 8, mix_group, jnp.zeros((HEAD_DIM, ROWS), F32))
        out_copy(v_buf, nv, vo_sem, head).start()
        return carry
    lax.fori_loop(0, HEADS, head_step, 0)

    mixed = jnp.concatenate([jnp.transpose(mix[block * 128:(block + 1) * 128, :]).astype(BF16)
                             for block in range(FLAT // 128)], axis=1)
    wo_copy.wait()

    def o_step(block, carry):
        cols = pl.ds(pl.multiple_of(block * 512, 512), 512)
        value = jnp.dot(mixed, wo_buf[:, cols], preferred_element_type=F32)
        part_ref[:, :, cols] = value.reshape(16, 8, 512).astype(BF16)
        return carry
    lax.fori_loop(0, D_MODEL // 512, o_step, 0)

    def end_out(head, carry):
        out_copy(k_buf, nk, ko_sem, head).wait()
        out_copy(v_buf, nv, vo_sem, head).wait()
        return carry
    lax.fori_loop(0, HEADS, end_out, 0)


def self_stage(x_in, tok_row, rel_t, norm_row, w_q, w_k, w_v, w_o, sk_t, sv_t):
    hbm = pl.BlockSpec(memory_space=pl.ANY)
    vmem = pl.BlockSpec(memory_space=pltpu.VMEM)
    cache = jax.ShapeDtypeStruct((T_LEN, HEADS, HEAD_DIM, ROWS), BF16)
    dma = pltpu.SemaphoreType.DMA
    return pl.pallas_call(
        self_kernel,
        out_shape=(jax.ShapeDtypeStruct((16, 8, D_MODEL), BF16), cache, cache),
        in_specs=[hbm, vmem, vmem, vmem] + [hbm] * 6,
        out_specs=(vmem, hbm, hbm),
        scratch_shapes=[
            pltpu.VMEM((ROWS, D_MODEL), BF16), pltpu.VMEM((ROWS, D_MODEL), BF16),
            pltpu.VMEM((D_MODEL, 3 * FLAT), BF16), pltpu.VMEM((FLAT, D_MODEL), BF16),
            pltpu.VMEM((HEADS, T_LEN, HEAD_DIM, ROWS), BF16), pltpu.VMEM((HEADS, T_LEN, HEAD_DIM, ROWS), BF16),
            pltpu.VMEM((ROWS, 3 * FLAT), F32), pltpu.VMEM((FLAT, ROWS), F32),
            pltpu.VMEM((FLAT, ROWS), BF16), pltpu.VMEM((FLAT, ROWS), BF16),
            pltpu.VMEM((HEADS, T_LEN, ROWS), F32), pltpu.VMEM((T_LEN, ROWS), F32), pltpu.VMEM((FLAT, ROWS), F32),
            dma, dma((N_CHUNK, 3)), dma, dma((HEADS,)), dma((HEADS,)), dma((HEADS,)), dma((HEADS,)),
        ],
        compiler_params=pltpu.CompilerParams(vmem_limit_bytes=56 * 1024 * 1024),
        cost_estimate=pl.CostEstimate(flops=10 ** 9, bytes_accessed=50 * 2 ** 20, transcendentals=0),
        name='self_stage',
    )(x_in, tok_row, rel_t, norm_row, w_q, w_k, w_v, w_o, sk_t, sv_t)


GROUPS = 2
GROUP_ROWS = ROWS // GROUPS
OWN = GROUP_ROWS // 8
STEP_ROWS = 8
STEPS = ROWS // STEP_ROWS
GROUP_STEPS = STEPS // GROUPS
SLOTS = 9
PAIR = 2 * HEADS
MESH = pl.DeviceIdType.MESH


def layer_kernel(part_in, x_hbm, enc_ref, nc_ref, nm_ref, ck, cv, wcq, wco, wg, wu, wd,
                 out_ref,
                 x_own, g_buf, u_buf, d_buf, co_buf, k_buf, v_buf, part, d2d_buf, chip_sum, rs_buf, h_full,
                 h_rows, resid, q_buf, mixed, hidden, mask_buf,
                 x_sem, cq_sem, co_sem, g_sem, u_sem, d_sem, k_sem, v_sem,
                 dd_send, dd_recv, rs_send, rs_recv, ag_send, ag_recv, fw_send, fw_recv):
    me = lax.axis_index('tp')
    core = me % 2
    chip = me // 2
    partner = me + 1 - 2 * core
    chips = (chip + 1 - 2 * (chip % 2), (chip + 2) % 4, 3 - chip)
    peers = tuple(other * 2 + core for other in chips)

    barrier = pltpu.get_barrier_semaphore()
    for dev in (partner,) + peers:
        pl.semaphore_signal(barrier, inc=1, device_id={'tp': dev}, device_id_type=MESH)

    def block(group, half, which):
        return group * 8 + half * 4 + which

    x_copies = [pltpu.make_async_copy(x_hbm.at[block(g, core, chip)], x_own.at[g], x_sem.at[g]) for g in range(GROUPS)]
    cq_copy = pltpu.make_async_copy(wcq, g_buf.at[:, pl.ds(0, FLAT)], cq_sem)
    co_copy = pltpu.make_async_copy(wco, co_buf, co_sem)
    g_copy = pltpu.make_async_copy(wg, g_buf, g_sem)
    u_copy = pltpu.make_async_copy(wu, u_buf, u_sem)
    d_copy = pltpu.make_async_copy(wd, d_buf, d_sem)
    step_len = STEP_ROWS * FLAT

    def kv_copies(step):
        slot = step % SLOTS
        span = pl.ds(pl.multiple_of(step * step_len, step_len), step_len)
        return (pltpu.make_async_copy(ck.at[span, :], k_buf.at[slot], k_sem.at[slot]),
                pltpu.make_async_copy(cv.at[span, :], v_buf.at[slot], v_sem.at[slot]))

    def kv_start(step, carry=0):
        for copy in kv_copies(step):
            copy.start()
        return carry

    for copy in x_copies:
        copy.start()
    cq_copy.start()
    lax.fori_loop(0, SLOTS, kv_start, 0)
    co_copy.start()
    u_copy.start()
    d_copy.start()

    mask_buf[...] = jnp.where(enc_ref[...] != 0, 0.0, NEG_FILL)
    pl.semaphore_wait(barrier, 4)

    def d2d(group, src):
        return pltpu.make_async_remote_copy(
            src_ref=src.at[pl.ds(block(group, 1 - core, 0), 4)], dst_ref=d2d_buf.at[group],
            send_sem=dd_send.at[group], recv_sem=dd_recv.at[group], device_id={'tp': partner}, device_id_type=MESH)

    def scatter(group, j):
        return pltpu.make_async_remote_copy(
            src_ref=chip_sum.at[group, chips[j]], dst_ref=rs_buf.at[group, j],
            send_sem=rs_send.at[group, j], recv_sem=rs_recv.at[group, j],
            device_id={'tp': peers[j]}, device_id_type=MESH)

    def gather(group, j):
        own = block(group, core, chip)
        return pltpu.make_async_remote_copy(
            src_ref=h_full.at[own], dst_ref=h_full.at[own],
            send_sem=ag_send.at[group, j], recv_sem=ag_recv.at[group, j],
            device_id={'tp': peers[j]}, device_id_type=MESH)

    def forward(group, j):
        piece = block(group, core, chip if j == 3 else chips[j])
        return pltpu.make_async_remote_copy(
            src_ref=h_full.at[piece], dst_ref=h_full.at[piece],
            send_sem=fw_send.at[group, j], recv_sem=fw_recv.at[group, j],
            device_id={'tp': partner}, device_id_type=MESH)

    def reduce_chip(group, src):
        d2d(group, src).wait()
        for which in (3, 2, 1, 0):
            total = (src[block(group, core, which)].astype(F32) + d2d_buf[group, which].astype(F32))
            chip_sum[group, which] = total.astype(BF16)
        for j in (2, 0, 1):
            scatter(group, j).start()

    def finish_rows(group, norm_row, last):
        total = resid[group] + chip_sum[group, chip].astype(F32)
        for j in range(3):
            scatter(group, j).wait()
            total = total + rs_buf[group, j].astype(F32)
        resid[group] = total
        own = block(group, core, chip)
        h_full[own] = total.astype(BF16) if last else rms_norm(total, norm_row[...].astype(F32))
        for j in (2, 0, 1):
            gather(group, j).start()
        forward(group, 3).start()

    def pass_on(group):
        for j in (0, 1, 2):
            gather(group, j).wait()
            forward(group, j).start()

    def rows_ready(group):
        for j in (3, 0, 1, 2):
            forward(group, j).wait()

    def collect(group):
        rows_ready(group)

        def two(i, carry):
            pair = h_full[pl.ds(group * 8 + i * 2, 2)].astype(F32).reshape(16, D_MODEL)
            h_rows[pl.ds(pl.multiple_of(group * GROUP_ROWS + i * 16, 16), 16), :] = pair.astype(BF16)
            return carry
        lax.fori_loop(0, GROUP_ROWS // 16, two, 0)

    def out_product(group, left, weight_ref):
        def cols_step(i, carry):
            cols = pl.ds(pl.multiple_of(i * 512, 512), 512)
            value = jnp.dot(left(), weight_ref[:, cols], preferred_element_type=F32)
            part[pl.ds(group * 8, 8), :, cols] = value.reshape(8, OWN, 512).astype(BF16)
            return carry
        lax.fori_loop(0, D_MODEL // 512, cols_step, 0)

    own_head = (lax.broadcasted_iota(jnp.int32, (HEADS, FLAT), 1) // HEAD_DIM
                == lax.broadcasted_iota(jnp.int32, (HEADS, FLAT), 0))

    def queries(group):
        span = slice(group * GROUP_ROWS, (group + 1) * GROUP_ROWS)
        value = jnp.dot(h_rows[span, :], g_buf[:, :FLAT], preferred_element_type=F32)
        q_buf[span, :] = value.astype(BF16).astype(F32)

    def cross_step(step):
        slot = step % SLOTS
        k_copy, v_copy = kv_copies(step)
        k_copy.wait()
        base = pl.multiple_of(step * STEP_ROWS, STEP_ROWS)
        q_rows = q_buf[pl.ds(base, STEP_ROWS), :]
        mask_rows = mask_buf[pl.ds(base, STEP_ROWS), :]
        scores = []
        for pair in range(STEP_ROWS // 2):
            left = jnp.concatenate([jnp.where(own_head, q_rows[2 * pair + i:2 * pair + i + 1, :], 0.0) for i in range(2)], axis=0)
            keys = jnp.concatenate([k_buf[slot, (2 * pair + i) * FLAT:(2 * pair + i + 1) * FLAT, :] for i in range(2)], axis=1)
            both = jnp.dot(left.astype(BF16), keys, preferred_element_type=F32)
            scores.append(both[:HEADS, :S_LEN] + mask_rows[2 * pair:2 * pair + 1, :])
            scores.append(both[HEADS:, S_LEN:] + mask_rows[2 * pair + 1:2 * pair + 2, :])
        score = jnp.concatenate(scores, axis=0)
        weight = jnp.exp(score - jnp.max(score, axis=1, keepdims=True))
        weight = weight / jnp.sum(weight, axis=1, keepdims=True)
        v_copy.wait()
        zeros = jnp.zeros((HEADS, S_LEN), F32)
        rows = []
        for pair in range(STEP_ROWS // 2):
            first = weight[2 * pair * HEADS:(2 * pair + 1) * HEADS, :]
            second = weight[(2 * pair + 1) * HEADS:(2 * pair + 2) * HEADS, :]
            left = jnp.concatenate([jnp.concatenate([first, zeros], axis=1), jnp.concatenate([zeros, second], axis=1)], axis=0)
            vals = jnp.concatenate([v_buf[slot, (2 * pair + i) * FLAT:(2 * pair + i + 1) * FLAT, :] for i in range(2)], axis=1)
            both = lax.dot_general(left.astype(BF16), vals, (((1,), (1,)), ((), ())), preferred_element_type=F32)
            for i in range(2):
                mine = jnp.where(own_head, both[i * HEADS:(i + 1) * HEADS, :], 0.0)
                rows.append(jnp.sum(mine, axis=0, keepdims=True))
        mixed[pl.ds(base, STEP_ROWS), :] = jnp.concatenate(rows, axis=0)

    def cross_out(group):
        span = slice(group * GROUP_ROWS, (group + 1) * GROUP_ROWS)
        out_product(group, lambda: mixed[span, :].astype(BF16), co_buf)

    def mlp_in(group, at_block):
        span = slice(group * GROUP_ROWS, (group + 1) * GROUP_ROWS)

        def unit_step(i, carry):
            at_block(i)
            cols = pl.ds(pl.multiple_of(i * 256, 256), 256)
            gate = jnp.dot(h_rows[span, :], g_buf[:, cols], preferred_element_type=F32)
            up = jnp.dot(h_rows[span, :], u_buf[:, cols], preferred_element_type=F32)
            hidden[:, cols] = (jax.nn.gelu(gate, approximate=True) * up).astype(BF16)
            return carry
        lax.fori_loop(0, UNITS // 256, unit_step, 0)

    def mlp_out(group):
        out_product(group, lambda: hidden[...], d_buf)

    for g in range(GROUPS):
        d2d(g, part_in).start()
    for g in range(GROUPS):
        reduce_chip(g, part_in)
    for g in range(GROUPS):
        x_copies[g].wait()
        resid[g] = x_own[g].astype(F32)
        finish_rows(g, nc_ref, False)
    pass_on(0)
    cq_copy.wait()
    collect(0)
    queries(0)

    def first_group(i, carry):
        @pl.when(i == 3)
        def _():
            pass_on(1)
            collect(1)
            queries(1)
            g_copy.start()
        cross_step(i)

        @pl.when(i < STEPS - SLOTS)
        def _():
            kv_start(i + SLOTS)
        return carry
    lax.fori_loop(0, GROUP_STEPS, first_group, 0)
    co_copy.wait()
    cross_out(0)
    d2d(0, part).start()

    def second_group(i, carry):
        @pl.when(i == 2)
        def _():
            reduce_chip(0, part)

        @pl.when(i == 6)
        def _():
            finish_rows(0, nm_ref, False)
        cross_step(i + GROUP_STEPS)
        return carry
    lax.fori_loop(0, GROUP_STEPS, second_group, 0)
    cross_out(1)
    d2d(1, part).start()
    pass_on(0)
    reduce_chip(1, part)
    collect(0)
    g_copy.wait()
    u_copy.wait()
    d_copy.wait()

    def mid_first(i):
        @pl.when(i == 3)
        def _():
            finish_rows(1, nm_ref, False)
    mlp_in(0, mid_first)
    mlp_out(0)
    d2d(0, part).start()
    pass_on(1)
    collect(1)

    def mid_second(i):
        @pl.when(i == 1)
        def _():
            reduce_chip(0, part)
    mlp_in(1, mid_second)
    mlp_out(1)
    d2d(1, part).start()
    finish_rows(0, nm_ref, True)
    reduce_chip(1, part)
    pass_on(0)
    finish_rows(1, nm_ref, True)
    rows_ready(0)
    out_ref[0:8] = h_full[0:8]
    pass_on(1)
    rows_ready(1)
    out_ref[8:16] = h_full[8:16]


def layer_stage(part, x_blocks, enc_mask, norm_cross, norm_mlp, ck, cv, cross_q, cross_o, w_gate, w_up, w_down):
    hbm = pl.BlockSpec(memory_space=pl.ANY)
    vmem = pl.BlockSpec(memory_space=pltpu.VMEM)
    dma = pltpu.SemaphoreType.DMA
    blocks = (2 * 8, OWN, D_MODEL)
    return pl.pallas_call(
        layer_kernel,
        out_shape=jax.ShapeDtypeStruct(blocks, BF16),
        in_specs=[vmem, hbm, vmem, vmem, vmem] + [hbm] * 7,
        out_specs=vmem,
        scratch_shapes=[
            pltpu.VMEM((GROUPS, OWN, D_MODEL), BF16),
            pltpu.VMEM((D_MODEL, UNITS), BF16), pltpu.VMEM((D_MODEL, UNITS), BF16), pltpu.VMEM((UNITS, D_MODEL), BF16),
            pltpu.VMEM((FLAT, D_MODEL), BF16),
            pltpu.VMEM((SLOTS, STEP_ROWS * FLAT, S_LEN), BF16), pltpu.VMEM((SLOTS, STEP_ROWS * FLAT, S_LEN), BF16),
            pltpu.VMEM(blocks, BF16),
            pltpu.VMEM((GROUPS, 4, OWN, D_MODEL), BF16), pltpu.VMEM((GROUPS, 4, OWN, D_MODEL), BF16),
            pltpu.VMEM((GROUPS, 3, OWN, D_MODEL), BF16), pltpu.VMEM(blocks, BF16),
            pltpu.VMEM((ROWS, D_MODEL), BF16), pltpu.VMEM((GROUPS, OWN, D_MODEL), F32),
            pltpu.VMEM((ROWS, FLAT), F32), pltpu.VMEM((ROWS, FLAT), F32), pltpu.VMEM((GROUP_ROWS, UNITS), BF16),
            pltpu.VMEM((ROWS, S_LEN), F32),
            dma((GROUPS,)), dma, dma, dma, dma, dma, dma((SLOTS,)), dma((SLOTS,)),
            dma((GROUPS,)), dma((GROUPS,)), dma((GROUPS, 3)), dma((GROUPS, 3)), dma((GROUPS, 3)), dma((GROUPS, 3)),
            dma((GROUPS, 4)), dma((GROUPS, 4)),
        ],
        compiler_params=pltpu.CompilerParams(collective_id=0, has_side_effects=True, vmem_limit_bytes=67043328),
        cost_estimate=pl.CostEstimate(flops=10 ** 10, bytes_accessed=70 * 2 ** 20, transcendentals=0),
        name='layer_stage',
    )(part, x_blocks, enc_mask, norm_cross, norm_mlp, ck, cv, cross_q, cross_o, w_gate, w_up, w_down)


def solution(mesh):
    def local_layer(x_in, tok_pos, self_k, self_v, cross_k, cross_v, enc_mask, rel_bias, w_q, w_k, w_v, w_o, cross_q, cross_o, w_gate, w_up, w_down, norm_self, norm_cross, norm_mlp):
        part, new_k, new_v = self_stage(
            x_in, tok_pos.reshape(1, ROWS), rel_bias.T, norm_self.reshape(1, D_MODEL), w_q, w_k, w_v, w_o,
            jnp.transpose(self_k, (1, 2, 3, 0)), jnp.transpose(self_v, (1, 2, 3, 0)))
        new_self_k = jnp.transpose(new_k, (3, 0, 1, 2))
        new_self_v = jnp.transpose(new_v, (3, 0, 1, 2))
        ck = jnp.transpose(cross_k, (0, 2, 3, 1)).reshape(ROWS * FLAT, S_LEN)
        cv = jnp.transpose(cross_v, (0, 2, 3, 1)).reshape(ROWS * FLAT, S_LEN)
        out = layer_stage(part, x_in.reshape(2 * 8, OWN, D_MODEL), enc_mask, norm_cross.reshape(1, D_MODEL),
                          norm_mlp.reshape(1, D_MODEL), ck, cv, cross_q, cross_o, w_gate, w_up, w_down)
        return out.reshape(ROWS, D_MODEL), new_self_k, new_self_v

    cache_spec = P('dp', None, 'tp', None)
    split_cols = P(None, 'tp')
    split_rows = P('tp', None)
    in_specs = (P('dp', None), P('dp'), cache_spec, cache_spec, cache_spec, cache_spec, P('dp', None), P(None, 'tp'), split_cols, split_cols, split_cols, split_rows, split_cols, split_rows, split_cols, split_cols, split_rows, P(None), P(None), P(None))
    out_specs = (P('dp', None), cache_spec, cache_spec)
    return jax.shard_map(local_layer, mesh=mesh, in_specs=in_specs, out_specs=out_specs, check_vma=False)
```

```python
import math
import jax
import jax.numpy as jnp
import numpy as np
from jax import lax
from jax.experimental import pallas as pl
from jax.experimental.pallas import tpu as pltpu
from jax.sharding import PartitionSpec as P

F32 = jnp.float32
BF16 = jnp.bfloat16
BUCKET_EDGES = tuple(int(math.ceil(16.0 * 8.0 ** (bucket_step / 16.0))) for bucket_step in range(1, 16))
NEG_FILL = -1e30
ROWS, T_LEN, S_LEN, HEADS, HEAD_DIM = 128, 64, 128, 8, 64
D_MODEL, FLAT, UNITS = 4096, 512, 1280
K_CHUNK = 1024
N_CHUNK = D_MODEL // K_CHUNK


def rms_norm(values, norm_scale):
    inv_rms = lax.rsqrt(jnp.mean(values * values, axis=-1, keepdims=True) + 1e-6)
    return (values * inv_rms * norm_scale).astype(BF16)


def lane_row(blocks):
    rows = blocks.astype(F32)
    return jnp.concatenate([rows[i:i + 1, :] for i in range(rows.shape[0])], axis=1)


def bias_table(rel_bias_t, tok_row):
    step = lax.broadcasted_iota(jnp.int32, (T_LEN, 32), 0)
    bucket = lax.broadcasted_iota(jnp.int32, (T_LEN, 32), 1)
    distance = (T_LEN - 1) - step
    far = jnp.full_like(distance, 16)
    for edge in BUCKET_EDGES:
        far = far + (distance >= edge).astype(jnp.int32)
    own_bucket = jnp.where(distance < 16, distance, far)
    one_hot = (bucket == own_bucket).astype(F32)
    by_step = lax.dot_general(one_hot, rel_bias_t, (((1,), (1,)), ((), ())),
                              precision=lax.Precision.HIGHEST, preferred_element_type=F32)
    shift = (T_LEN - 1) - tok_row
    position = lax.broadcasted_iota(jnp.int32, (T_LEN, ROWS), 0)
    allowed = position <= tok_row
    tables = []
    for head in range(HEADS):
        table = jnp.broadcast_to(by_step[:, head:head + 1], (T_LEN, ROWS))
        for bit in (32, 16, 8, 4, 2, 1):
            moved = jnp.concatenate([table[bit:], table[:bit]], axis=0)
            table = jnp.where((shift & bit) != 0, moved, table)
        tables.append(jnp.where(allowed, table, NEG_FILL))
    return tables


def self_kernel(x_hbm, tok_ref, rel_ref, norm_ref, wq, wk, wv, wo, sk, sv,
                part_ref, nk, nv,
                x_buf, h_buf, w_buf, wo_buf, k_buf, v_buf, acc, q_t, kn_t, vn_t, bias, probs, mix, norm_row,
                x_sem, w_sem, wo_sem, k_sem, v_sem, ko_sem, vo_sem):
    x_copy = pltpu.make_async_copy(x_hbm, x_buf, x_sem)
    x_copy.start()
    srcs = (wq, wk, wv)

    def w_copy(chunk, which):
        rows = pl.ds(pl.multiple_of(chunk * K_CHUNK, K_CHUNK), K_CHUNK)
        return pltpu.make_async_copy(srcs[which].at[rows, :], w_buf.at[rows, pl.ds(which * FLAT, FLAT)],
                                     w_sem.at[chunk, which])

    def in_copy(src, buf, sem, head):
        return pltpu.make_async_copy(src.at[:, head], buf.at[head], sem.at[head])

    def out_copy(buf, dst, sem, head):
        return pltpu.make_async_copy(buf.at[head], dst.at[:, head], sem.at[head])

    for chunk in range(N_CHUNK):
        for which in range(3):
            w_copy(chunk, which).start()

    def start_in(head, carry):
        in_copy(sk, k_buf, k_sem, head).start()
        in_copy(sv, v_buf, v_sem, head).start()
        return carry
    lax.fori_loop(0, HEADS, start_in, 0)
    wo_copy = pltpu.make_async_copy(wo, wo_buf, wo_sem)
    wo_copy.start()

    tok_row = tok_ref[...]
    for head, table in enumerate(bias_table(rel_ref[...], tok_row)):
        bias[head] = table

    norm_row[...] = lane_row(norm_ref[...])
    x_copy.wait()

    def norm_rows(step, carry):
        rows = pl.ds(pl.multiple_of(step * 16, 16), 16)
        h_buf[rows, :] = rms_norm(x_buf[rows, :].astype(F32), norm_row[...])
        return carry
    lax.fori_loop(0, ROWS // 16, norm_rows, 0)

    acc[...] = jnp.zeros_like(acc)

    def qkv_step(chunk, carry):
        for which in range(3):
            w_copy(chunk, which).wait()
            rows = pl.ds(pl.multiple_of(chunk * K_CHUNK, K_CHUNK), K_CHUNK)
            cols = slice(which * FLAT, (which + 1) * FLAT)
            acc[:, cols] += jnp.dot(h_buf[:, rows], w_buf[rows, cols], preferred_element_type=F32)
        return carry
    lax.fori_loop(0, N_CHUNK, qkv_step, 0)

    for which, dst in enumerate((q_t, kn_t, vn_t)):
        for block in range(FLAT // 128):
            start = which * FLAT + block * 128
            turned = jnp.transpose(acc[:, start:start + 128])
            dst[block * 128:(block + 1) * 128, :] = turned.astype(BF16).astype(dst.dtype)

    tok_b = jnp.broadcast_to(tok_row.astype(F32), (HEAD_DIM, ROWS)).astype(BF16)

    def start_out(head, carry):
        out_copy(k_buf, nk, ko_sem, head).start()
        out_copy(v_buf, nv, vo_sem, head).start()
        return carry

    def head_step(head, carry):
        lanes = pl.ds(pl.multiple_of(head * HEAD_DIM, HEAD_DIM), HEAD_DIM)
        in_copy(sk, k_buf, k_sem, head).wait()
        query = q_t[lanes, :]
        fresh_k = kn_t[lanes, :]

        def score_group(group, inner):
            at_tok = tok_b - (group * 8).astype(F32).astype(BF16)
            rows = []
            for i in range(8):
                step = group * 8 + i
                keys = jnp.where(at_tok == jnp.asarray(i, BF16), fresh_k, k_buf[head, step])
                k_buf[head, step] = keys
                rows.append(jnp.sum(keys.astype(F32) * query, axis=0, keepdims=True))
            probs[pl.ds(pl.multiple_of(group * 8, 8), 8), :] = jnp.concatenate(rows, axis=0)
            return inner
        lax.fori_loop(0, T_LEN // 8, score_group, 0)
        scores = probs[...] + bias[head]
        weights = jnp.exp(scores - jnp.max(scores, axis=0, keepdims=True))
        weights = weights / jnp.sum(weights, axis=0, keepdims=True)
        probs[...] = weights.astype(BF16).astype(F32)
        in_copy(sv, v_buf, v_sem, head).wait()
        fresh_v = vn_t[lanes, :]

        def mix_group(group, total):
            at_tok = tok_b - (group * 8).astype(F32).astype(BF16)
            for i in range(8):
                step = group * 8 + i
                vals = jnp.where(at_tok == jnp.asarray(i, BF16), fresh_v, v_buf[head, step])
                v_buf[head, step] = vals
                total = total + vals.astype(F32) * probs[pl.ds(step, 1), :]
            return total
        mix[lanes, :] = lax.fori_loop(0, T_LEN // 8, mix_group, jnp.zeros((HEAD_DIM, ROWS), F32))

        start_out(head, 0)
        return carry
    lax.fori_loop(0, HEADS, head_step, 0)

    mixed = jnp.concatenate([jnp.transpose(mix[block * 128:(block + 1) * 128, :]).astype(BF16)
                             for block in range(FLAT // 128)], axis=1)
    wo_copy.wait()

    for start in range(0, D_MODEL, 1024):
        value = jnp.dot(mixed, wo_buf[:, start:start + 1024], preferred_element_type=F32)
        part_ref[:, :, start:start + 1024] = value.reshape(16, 8, 1024).astype(BF16)

    def end_out(head, carry):
        out_copy(k_buf, nk, ko_sem, head).wait()
        out_copy(v_buf, nv, vo_sem, head).wait()
        return carry
    lax.fori_loop(0, HEADS, end_out, 0)


def self_stage(x_in, tok_row, rel_t, norm_row, w_q, w_k, w_v, w_o, sk_t, sv_t):
    hbm = pl.BlockSpec(memory_space=pltpu.HBM)
    vmem = pl.BlockSpec(memory_space=pltpu.VMEM)
    cache = jax.ShapeDtypeStruct((T_LEN, HEADS, HEAD_DIM, ROWS), BF16)
    dma = pltpu.SemaphoreType.DMA
    return pl.pallas_call(
        self_kernel,
        out_shape=(jax.ShapeDtypeStruct((16, 8, D_MODEL), BF16), cache, cache),
        in_specs=[hbm, vmem, vmem, vmem] + [hbm] * 6,
        out_specs=(vmem, hbm, hbm),
        scratch_shapes=[
            pltpu.VMEM((ROWS, D_MODEL), BF16), pltpu.VMEM((ROWS, D_MODEL), BF16),
            pltpu.VMEM((D_MODEL, 3 * FLAT), BF16), pltpu.VMEM((FLAT, D_MODEL), BF16),
            pltpu.VMEM((HEADS, T_LEN, HEAD_DIM, ROWS), BF16), pltpu.VMEM((HEADS, T_LEN, HEAD_DIM, ROWS), BF16),
            pltpu.VMEM((ROWS, 3 * FLAT), F32), pltpu.VMEM((FLAT, ROWS), F32),
            pltpu.VMEM((FLAT, ROWS), BF16), pltpu.VMEM((FLAT, ROWS), BF16),
            pltpu.VMEM((HEADS, T_LEN, ROWS), F32), pltpu.VMEM((T_LEN, ROWS), F32), pltpu.VMEM((FLAT, ROWS), F32),
            pltpu.VMEM((1, D_MODEL), F32),
            dma, dma((N_CHUNK, 3)), dma, dma((HEADS,)), dma((HEADS,)), dma((HEADS,)), dma((HEADS,)),
        ],
        compiler_params=pltpu.CompilerParams(vmem_limit_bytes=60 * 1024 * 1024),
        cost_estimate=pl.CostEstimate(flops=10 ** 9, bytes_accessed=50 * 2 ** 20, transcendentals=0),
        name='self_stage',
    )(x_in, tok_row, rel_t, norm_row, w_q, w_k, w_v, w_o, sk_t, sv_t)


GROUPS = 2
GROUP_ROWS = ROWS // GROUPS
OWN = GROUP_ROWS // 8
STEP_ROWS = 16
SPLIT = 2
OUT_COLS = D_MODEL // SPLIT
STEPS = ROWS // STEP_ROWS
GROUP_STEPS = STEPS // GROUPS
SLOTS = 4
PAIR = 2 * HEADS
MESH = pl.DeviceIdType.MESH


def layer_kernel(part_in, x_hbm, enc_ref, nc_ref, nm_ref, ck, cv, wcq, wco, wg, wu, wd,
                 out_ref,
                 x_own, g_buf, u_buf, d_buf, co_buf, k_buf, v_buf, part, d2d_buf, chip_sum, rs_buf, h_full,
                 h_rows, resid, q_buf, mixed, hidden, mask_buf, norm_rows,
                 x_sem, cq_sem, co_sem, g_sem, u_sem, d_sem, k_sem, v_sem,
                 dd_send, dd_recv, rs_send, rs_recv, ag_send, ag_recv, fw_send, fw_recv):
    me = lax.axis_index('tp')
    core = me % 2
    chip = me // 2
    partner = me + 1 - 2 * core
    chips = (chip + 1 - 2 * (chip % 2), (chip + 2) % 4, 3 - chip)
    peers = tuple(other * 2 + core for other in chips)

    barrier = pltpu.get_barrier_semaphore()
    for dev in (partner,) + peers:
        pl.semaphore_signal(barrier, inc=1, device_id={'tp': dev}, device_id_type=MESH)

    def block(group, half, which):
        return group * 8 + half * 4 + which

    x_copies = [pltpu.make_async_copy(x_hbm.at[block(g, core, chip)], x_own.at[g], x_sem.at[g]) for g in range(GROUPS)]
    cq_copy = pltpu.make_async_copy(wcq, g_buf.at[:, pl.ds(0, FLAT)], cq_sem)
    co_copy = pltpu.make_async_copy(wco, co_buf, co_sem)
    g_copy = pltpu.make_async_copy(wg, g_buf, g_sem)
    u_copy = pltpu.make_async_copy(wu, u_buf, u_sem)
    d_copy = pltpu.make_async_copy(wd, d_buf, d_sem)
    step_len = STEP_ROWS * FLAT

    def kv_copies(step):
        slot = step % SLOTS
        span = pl.ds(pl.multiple_of(step * step_len, step_len), step_len)
        return (pltpu.make_async_copy(ck.at[span, :], k_buf.at[slot], k_sem.at[slot]),
                pltpu.make_async_copy(cv.at[span, :], v_buf.at[slot], v_sem.at[slot]))

    def kv_start(step, carry=0):
        for copy in kv_copies(step):
            copy.start()
        return carry

    for copy in x_copies:
        copy.start()
    cq_copy.start()
    lax.fori_loop(0, SLOTS, kv_start, 0)
    co_copy.start()
    u_copy.start()
    d_copy.start()

    norm_rows[0] = lane_row(nc_ref[...])
    norm_rows[1] = lane_row(nm_ref[...])
    mask_buf[...] = jnp.where(enc_ref[...] != 0, 0.0, NEG_FILL)
    pl.semaphore_wait(barrier, 4)

    def columns(part_no):
        return pl.ds(part_no * OUT_COLS, OUT_COLS)

    def d2d(group, src, part_no):
        return pltpu.make_async_remote_copy(
            src_ref=src.at[pl.ds(block(group, 1 - core, 0), 4), :, columns(part_no)],
            dst_ref=d2d_buf.at[group, :, :, columns(part_no)],
            send_sem=dd_send.at[group, part_no], recv_sem=dd_recv.at[group, part_no],
            device_id={'tp': partner}, device_id_type=MESH)

    def scatter(group, j, part_no):
        return pltpu.make_async_remote_copy(
            src_ref=chip_sum.at[group, chips[j], :, columns(part_no)], dst_ref=rs_buf.at[group, j, :, columns(part_no)],
            send_sem=rs_send.at[group, j, part_no], recv_sem=rs_recv.at[group, j, part_no],
            device_id={'tp': peers[j]}, device_id_type=MESH)

    def gather(group, j, rows_ref):
        own = block(group, core, chip)
        return pltpu.make_async_remote_copy(
            src_ref=rows_ref.at[own], dst_ref=rows_ref.at[own],
            send_sem=ag_send.at[group, j], recv_sem=ag_recv.at[group, j],
            device_id={'tp': peers[j]}, device_id_type=MESH)

    def forward(group, j, rows_ref):
        piece = block(group, core, chip if j == 3 else chips[j])
        return pltpu.make_async_remote_copy(
            src_ref=rows_ref.at[piece], dst_ref=rows_ref.at[piece],
            send_sem=fw_send.at[group, j], recv_sem=fw_recv.at[group, j],
            device_id={'tp': partner}, device_id_type=MESH)

    def d2d_start(group, src):
        for part_no in range(SPLIT):
            d2d(group, src, part_no).start()

    def reduce_chip(group, src):
        for part_no in range(SPLIT):
            d2d(group, src, part_no).wait()
            cols = columns(part_no)
            for which in range(4):
                total = src[block(group, core, which), :, cols].astype(F32) + d2d_buf[group, which, :, cols].astype(F32)
                chip_sum[group, which, :, cols] = total.astype(BF16)
            for j in (2, 0, 1):
                scatter(group, j, part_no).start()

    def finish_rows(group, norm, last):
        for part_no in range(SPLIT):
            cols = columns(part_no)
            total = resid[group, :, cols] + chip_sum[group, chip, :, cols].astype(F32)
            for j in range(3):
                scatter(group, j, part_no).wait()
                total = total + rs_buf[group, j, :, cols].astype(F32)
            resid[group, :, cols] = total
        own = block(group, core, chip)
        rows_ref = out_ref if last else h_full
        rows_ref[own] = resid[group].astype(BF16) if last else rms_norm(resid[group], norm_rows[norm])
        for j in (2, 0, 1):
            gather(group, j, rows_ref).start()
        forward(group, 3, rows_ref).start()

    def pass_on(group, rows_ref=h_full):
        for j in (0, 1, 2):
            gather(group, j, rows_ref).wait()
            forward(group, j, rows_ref).start()

    def rows_ready(group, rows_ref=h_full):
        for j in (3, 0, 1, 2):
            forward(group, j, rows_ref).wait()

    def collect(group):
        rows_ready(group)

        def two(i, carry):
            pair = h_full[pl.ds(group * 8 + i * 2, 2)].astype(F32).reshape(16, D_MODEL)
            h_rows[pl.ds(pl.multiple_of(group * GROUP_ROWS + i * 16, 16), 16), :] = pair.astype(BF16)
            return carry
        lax.fori_loop(0, GROUP_ROWS // 16, two, 0)

    def out_product(group, left, weight_ref):
        rows = left()
        for part_no in range(SPLIT):
            cols = slice(part_no * OUT_COLS, (part_no + 1) * OUT_COLS)
            value = jnp.dot(rows, weight_ref[:, cols], preferred_element_type=F32)
            part[group * 8:(group + 1) * 8, :, cols] = value.reshape(8, OWN, OUT_COLS).astype(BF16)
            d2d(group, part, part_no).start()

    own_head = (lax.broadcasted_iota(jnp.int32, (HEADS, FLAT), 1) // HEAD_DIM
                == lax.broadcasted_iota(jnp.int32, (HEADS, FLAT), 0))

    def queries(group):
        span = slice(group * GROUP_ROWS, (group + 1) * GROUP_ROWS)
        value = jnp.dot(h_rows[span, :], g_buf[:, :FLAT], preferred_element_type=F32)
        q_buf[span, :] = value.astype(BF16).astype(F32)

    def cross_step(step):
        slot = step % SLOTS
        k_copy, v_copy = kv_copies(step)
        k_copy.wait()
        base = pl.multiple_of(step * STEP_ROWS, STEP_ROWS)
        q_rows = q_buf[pl.ds(base, STEP_ROWS), :]
        mask_rows = mask_buf[pl.ds(base, STEP_ROWS), :]
        scores = []
        for pair in range(STEP_ROWS // 2):
            left = jnp.concatenate([jnp.where(own_head, q_rows[2 * pair + i:2 * pair + i + 1, :], 0.0) for i in range(2)], axis=0)
            keys = jnp.concatenate([k_buf[slot, (2 * pair + i) * FLAT:(2 * pair + i + 1) * FLAT, :] for i in range(2)], axis=1)
            both = jnp.dot(left.astype(BF16), keys, preferred_element_type=F32)
            scores.append(both[:HEADS, :S_LEN] + mask_rows[2 * pair:2 * pair + 1, :])
            scores.append(both[HEADS:, S_LEN:] + mask_rows[2 * pair + 1:2 * pair + 2, :])
        score = jnp.concatenate(scores, axis=0)
        weight = jnp.exp(score - jnp.max(score, axis=1, keepdims=True))
        weight = weight / jnp.sum(weight, axis=1, keepdims=True)
        v_copy.wait()
        zeros = jnp.zeros((HEADS, S_LEN), F32)
        rows = []
        for pair in range(STEP_ROWS // 2):
            first = weight[2 * pair * HEADS:(2 * pair + 1) * HEADS, :]
            second = weight[(2 * pair + 1) * HEADS:(2 * pair + 2) * HEADS, :]
            left = jnp.concatenate([jnp.concatenate([first, zeros], axis=1), jnp.concatenate([zeros, second], axis=1)], axis=0)
            vals = jnp.concatenate([v_buf[slot, (2 * pair + i) * FLAT:(2 * pair + i + 1) * FLAT, :] for i in range(2)], axis=1)
            both = lax.dot_general(left.astype(BF16), vals, (((1,), (1,)), ((), ())), preferred_element_type=F32)
            for i in range(2):
                mine = jnp.where(own_head, both[i * HEADS:(i + 1) * HEADS, :], 0.0)
                rows.append(jnp.sum(mine, axis=0, keepdims=True))
        mixed[pl.ds(base, STEP_ROWS), :] = jnp.concatenate(rows, axis=0)

    def cross_out(group):
        span = slice(group * GROUP_ROWS, (group + 1) * GROUP_ROWS)
        out_product(group, lambda: mixed[span, :].astype(BF16), co_buf)

    def mlp_in(group, at_block):
        span = slice(group * GROUP_ROWS, (group + 1) * GROUP_ROWS)

        def unit_step(i, carry):
            at_block(i)
            cols = pl.ds(pl.multiple_of(i * 256, 256), 256)
            gate = jnp.dot(h_rows[span, :], g_buf[:, cols], preferred_element_type=F32)
            up = jnp.dot(h_rows[span, :], u_buf[:, cols], preferred_element_type=F32)
            hidden[:, cols] = (jax.nn.gelu(gate, approximate=True) * up).astype(BF16)
            return carry
        lax.fori_loop(0, UNITS // 256, unit_step, 0)

    def mlp_out(group):
        out_product(group, lambda: hidden[...], d_buf)

    for g in range(GROUPS):
        d2d_start(g, part_in)
    for g in range(GROUPS):
        reduce_chip(g, part_in)
    for g in range(GROUPS):
        x_copies[g].wait()
        resid[g] = x_own[g].astype(F32)
        finish_rows(g, 0, False)
    pass_on(0)
    cq_copy.wait()
    collect(0)
    queries(0)

    def first_group(i, carry):
        cross_step(i)

        @pl.when(i < STEPS - SLOTS)
        def _():
            kv_start(i + SLOTS)
        return carry
    lax.fori_loop(0, 3, first_group, 0)
    pass_on(1)
    lax.fori_loop(3, GROUP_STEPS, first_group, 0)
    co_copy.wait()
    cross_out(0)
    collect(1)
    queries(1)
    g_copy.start()

    def second_group(i, carry):
        @pl.when(i == 1)
        def _():
            reduce_chip(0, part)
        cross_step(i + GROUP_STEPS)
        return carry
    lax.fori_loop(0, GROUP_STEPS, second_group, 0)
    cross_out(1)
    finish_rows(0, 1, False)
    reduce_chip(1, part)
    pass_on(0)
    collect(0)
    g_copy.wait()
    u_copy.wait()
    d_copy.wait()

    def mid_first(i):
        @pl.when(i == 0)
        def _():
            finish_rows(1, 1, False)
    mlp_in(0, mid_first)
    pass_on(1)
    mlp_out(0)
    collect(1)

    def mid_second(i):
        @pl.when(i == 1)
        def _():
            reduce_chip(0, part)
    mlp_in(1, mid_second)
    finish_rows(0, 1, True)
    mlp_out(1)
    reduce_chip(1, part)
    pass_on(0, out_ref)
    finish_rows(1, 1, True)
    rows_ready(0, out_ref)
    pass_on(1, out_ref)
    rows_ready(1, out_ref)


def layer_stage(part, x_blocks, enc_mask, norm_cross, norm_mlp, ck, cv, cross_q, cross_o, w_gate, w_up, w_down):
    hbm = pl.BlockSpec(memory_space=pltpu.HBM)
    vmem = pl.BlockSpec(memory_space=pltpu.VMEM)
    dma = pltpu.SemaphoreType.DMA
    blocks = (2 * 8, OWN, D_MODEL)
    return pl.pallas_call(
        layer_kernel,
        out_shape=jax.ShapeDtypeStruct(blocks, BF16),
        in_specs=[vmem, hbm, vmem, vmem, vmem] + [hbm] * 7,
        out_specs=vmem,
        scratch_shapes=[
            pltpu.VMEM((GROUPS, OWN, D_MODEL), BF16),
            pltpu.VMEM((D_MODEL, UNITS), BF16), pltpu.VMEM((D_MODEL, UNITS), BF16), pltpu.VMEM((UNITS, D_MODEL), BF16),
            pltpu.VMEM((FLAT, D_MODEL), BF16),
            pltpu.VMEM((SLOTS, STEP_ROWS * FLAT, S_LEN), BF16), pltpu.VMEM((SLOTS, STEP_ROWS * FLAT, S_LEN), BF16),
            pltpu.VMEM(blocks, BF16),
            pltpu.VMEM((GROUPS, 4, OWN, D_MODEL), BF16), pltpu.VMEM((GROUPS, 4, OWN, D_MODEL), BF16),
            pltpu.VMEM((GROUPS, 3, OWN, D_MODEL), BF16), pltpu.VMEM(blocks, BF16),
            pltpu.VMEM((ROWS, D_MODEL), BF16), pltpu.VMEM((GROUPS, OWN, D_MODEL), F32),
            pltpu.VMEM((ROWS, FLAT), F32), pltpu.VMEM((ROWS, FLAT), F32), pltpu.VMEM((GROUP_ROWS, UNITS), BF16),
            pltpu.VMEM((ROWS, S_LEN), F32), pltpu.VMEM((2, 1, D_MODEL), F32),
            dma((GROUPS,)), dma, dma, dma, dma, dma, dma((SLOTS,)), dma((SLOTS,)),
            dma((GROUPS, SPLIT)), dma((GROUPS, SPLIT)), dma((GROUPS, 3, SPLIT)), dma((GROUPS, 3, SPLIT)),
            dma((GROUPS, 3)), dma((GROUPS, 3)),
            dma((GROUPS, 4)), dma((GROUPS, 4)),
        ],
        compiler_params=pltpu.CompilerParams(collective_id=0, has_side_effects=True, vmem_limit_bytes=59 * 1024 * 1024),
        cost_estimate=pl.CostEstimate(flops=10 ** 10, bytes_accessed=70 * 2 ** 20, transcendentals=0),
        name='layer_stage',
    )(part, x_blocks, enc_mask, norm_cross, norm_mlp, ck, cv, cross_q, cross_o, w_gate, w_up, w_down)


def solution(mesh):
    def local_layer(x_in, tok_pos, self_k, self_v, cross_k, cross_v, enc_mask, rel_bias, w_q, w_k, w_v, w_o, cross_q, cross_o, w_gate, w_up, w_down, norm_self, norm_cross, norm_mlp):
        part, new_k, new_v = self_stage(
            x_in, tok_pos.reshape(1, ROWS), rel_bias.T, norm_self.reshape(32, 128), w_q, w_k, w_v, w_o,
            jnp.transpose(self_k, (1, 2, 3, 0)), jnp.transpose(self_v, (1, 2, 3, 0)))
        new_self_k = jnp.transpose(new_k, (3, 0, 1, 2))
        new_self_v = jnp.transpose(new_v, (3, 0, 1, 2))
        ck = jnp.transpose(cross_k, (0, 2, 3, 1)).reshape(ROWS * FLAT, S_LEN)
        cv = jnp.transpose(cross_v, (0, 2, 3, 1)).reshape(ROWS * FLAT, S_LEN)
        out = layer_stage(part, x_in.reshape(2 * 8, OWN, D_MODEL), enc_mask, norm_cross.reshape(32, 128),
                          norm_mlp.reshape(32, 128), ck, cv, cross_q, cross_o, w_gate, w_up, w_down)
        return out.reshape(ROWS, D_MODEL), new_self_k, new_self_v

    cache_spec = P('dp', None, 'tp', None)
    split_cols = P(None, 'tp')
    split_rows = P('tp', None)
    in_specs = (P('dp', None), P('dp'), cache_spec, cache_spec, cache_spec, cache_spec, P('dp', None), P(None, 'tp'), split_cols, split_cols, split_cols, split_rows, split_cols, split_rows, split_cols, split_cols, split_rows, P(None), P(None), P(None))
    out_specs = (P('dp', None), cache_spec, cache_spec)
    return jax.shard_map(local_layer, mesh=mesh, in_specs=in_specs, out_specs=out_specs, check_vma=False)
```

```python
import math
import jax
import jax.numpy as jnp
import numpy as np
from jax import lax
from jax.experimental import pallas as pl
from jax.experimental.pallas import tpu as pltpu
from jax.sharding import PartitionSpec as P

F32 = jnp.float32
BF16 = jnp.bfloat16
BUCKET_EDGES = tuple(int(math.ceil(16.0 * 8.0 ** (bucket_step / 16.0))) for bucket_step in range(1, 16))
NEG_FILL = -1e30
ROWS, T_LEN, S_LEN, HEADS, HEAD_DIM = 128, 64, 128, 8, 64
D_MODEL, FLAT, UNITS = 4096, 512, 1280
K_CHUNK = 1024
N_CHUNK = D_MODEL // K_CHUNK


def rms_norm(values, norm_scale):
    inv_rms = lax.rsqrt(jnp.mean(values * values, axis=-1, keepdims=True) + 1e-6)
    return (values * inv_rms * norm_scale).astype(BF16)


def lane_row(blocks):
    rows = blocks.astype(F32)
    return jnp.concatenate([rows[i:i + 1, :] for i in range(rows.shape[0])], axis=1)


def bias_table(rel_bias_t, tok_row):
    step = lax.broadcasted_iota(jnp.int32, (T_LEN, 32), 0)
    bucket = lax.broadcasted_iota(jnp.int32, (T_LEN, 32), 1)
    distance = (T_LEN - 1) - step
    far = jnp.full_like(distance, 16)
    for edge in BUCKET_EDGES:
        far = far + (distance >= edge).astype(jnp.int32)
    own_bucket = jnp.where(distance < 16, distance, far)
    one_hot = (bucket == own_bucket).astype(F32)
    by_step = lax.dot_general(one_hot, rel_bias_t, (((1,), (1,)), ((), ())),
                              precision=lax.Precision.HIGHEST, preferred_element_type=F32)
    shift = (T_LEN - 1) - tok_row
    position = lax.broadcasted_iota(jnp.int32, (T_LEN, ROWS), 0)
    allowed = position <= tok_row
    tables = []
    for head in range(HEADS):
        table = jnp.broadcast_to(by_step[:, head:head + 1], (T_LEN, ROWS))
        for bit in (32, 16, 8, 4, 2, 1):
            moved = jnp.concatenate([table[bit:], table[:bit]], axis=0)
            table = jnp.where((shift & bit) != 0, moved, table)
        tables.append(jnp.where(allowed, table, NEG_FILL))
    return tables


def self_kernel(x_hbm, tok_ref, rel_ref, norm_ref, wq, wk, wv, wo, sk, sv,
                part_ref, nk, nv,
                x_buf, h_buf, w_buf, wo_buf, k_buf, v_buf, acc, q_t, kn_t, vn_t, bias, probs, mix, norm_row,
                x_sem, w_sem, wo_sem, k_sem, v_sem, ko_sem, vo_sem):
    x_copy = pltpu.make_async_copy(x_hbm, x_buf, x_sem)
    x_copy.start()
    srcs = (wq, wk, wv)

    def w_copy(chunk, which):
        rows = pl.ds(pl.multiple_of(chunk * K_CHUNK, K_CHUNK), K_CHUNK)
        return pltpu.make_async_copy(srcs[which].at[rows, :], w_buf.at[rows, pl.ds(which * FLAT, FLAT)],
                                     w_sem.at[chunk, which])

    def span(group):
        return pl.ds(pl.multiple_of(group * 8, 8), 8)

    def in_copy(src, buf, sem, group):
        return pltpu.make_async_copy(src.at[span(group)], buf.at[span(group)], sem.at[group])

    def out_copy(buf, dst, sem, group):
        return pltpu.make_async_copy(buf.at[span(group)], dst.at[span(group)], sem.at[group])

    for chunk in range(1):
        for which in range(3):
            w_copy(chunk, which).start()

    wo_copy = pltpu.make_async_copy(wo, wo_buf, wo_sem)

    tok_row = tok_ref[...]
    for head, table in enumerate(bias_table(rel_ref[...], tok_row)):
        bias[head] = table

    norm_row[...] = lane_row(norm_ref[...])
    x_copy.wait()
    for chunk in range(1, N_CHUNK):
        for which in range(3):
            w_copy(chunk, which).start()

    def norm_rows(step, carry):
        rows = pl.ds(pl.multiple_of(step * 16, 16), 16)
        h_buf[rows, :] = rms_norm(x_buf[rows, :].astype(F32), norm_row[...])
        return carry
    lax.fori_loop(0, ROWS // 16, norm_rows, 0)

    acc[...] = jnp.zeros_like(acc)

    def qkv_step(chunk, carry):
        for which in range(3):
            w_copy(chunk, which).wait()
            rows = pl.ds(pl.multiple_of(chunk * K_CHUNK, K_CHUNK), K_CHUNK)
            cols = slice(which * FLAT, (which + 1) * FLAT)
            acc[:, cols] += jnp.dot(h_buf[:, rows], w_buf[rows, cols], preferred_element_type=F32)

        @pl.when(chunk == 0)
        def _():
            for src, buf, sem in ((sk, k_buf, k_sem), (sv, v_buf, v_sem)):
                for group in range(T_LEN // 8):
                    in_copy(src, buf, sem, group).start()
            wo_copy.start()
        return carry
    lax.fori_loop(0, N_CHUNK, qkv_step, 0)

    for which, dst in enumerate((q_t, kn_t, vn_t)):
        for block in range(FLAT // 128):
            start = which * FLAT + block * 128
            turned = jnp.transpose(acc[:, start:start + 128])
            dst[block * 128:(block + 1) * 128, :] = turned.astype(BF16).astype(dst.dtype)

    tok_b = jnp.broadcast_to(tok_row.astype(F32), (HEAD_DIM, ROWS)).astype(BF16)

    def score_group(group, carry):
        in_copy(sk, k_buf, k_sem, group).wait()
        at_tok = tok_b - (group * 8).astype(F32).astype(BF16)

        def per_head(head, inner):
            lanes = pl.ds(pl.multiple_of(head * HEAD_DIM, HEAD_DIM), HEAD_DIM)
            query = q_t[lanes, :]
            fresh_k = kn_t[lanes, :]
            rows = []
            for i in range(8):
                step = group * 8 + i
                keys = jnp.where(at_tok == jnp.asarray(i, BF16), fresh_k, k_buf[step, head])
                k_buf[step, head] = keys
                rows.append(jnp.sum(keys.astype(F32) * query, axis=0, keepdims=True))
            probs[head, span(group), :] = jnp.concatenate(rows, axis=0)
            return inner
        lax.fori_loop(0, HEADS, per_head, 0)
        out_copy(k_buf, nk, ko_sem, group).start()
        return carry
    lax.fori_loop(0, T_LEN // 8, score_group, 0)

    def soften(head, carry):
        scores = probs[head] + bias[head]
        weights = jnp.exp(scores - jnp.max(scores, axis=0, keepdims=True))
        weights = weights / jnp.sum(weights, axis=0, keepdims=True)
        probs[head] = weights.astype(BF16).astype(F32)
        return carry
    lax.fori_loop(0, HEADS, soften, 0)
    mix[...] = jnp.zeros_like(mix)

    def mix_group(group, carry):
        in_copy(sv, v_buf, v_sem, group).wait()
        at_tok = tok_b - (group * 8).astype(F32).astype(BF16)

        def per_head(head, inner):
            lanes = pl.ds(pl.multiple_of(head * HEAD_DIM, HEAD_DIM), HEAD_DIM)
            fresh_v = vn_t[lanes, :]
            total = mix[lanes, :]
            for i in range(8):
                step = group * 8 + i
                vals = jnp.where(at_tok == jnp.asarray(i, BF16), fresh_v, v_buf[step, head])
                v_buf[step, head] = vals
                total = total + vals.astype(F32) * probs[head, pl.ds(step, 1), :]
            mix[lanes, :] = total
            return inner
        lax.fori_loop(0, HEADS, per_head, 0)
        out_copy(v_buf, nv, vo_sem, group).start()
        return carry
    lax.fori_loop(0, T_LEN // 8, mix_group, 0)

    mixed = jnp.concatenate([jnp.transpose(mix[block * 128:(block + 1) * 128, :]).astype(BF16)
                             for block in range(FLAT // 128)], axis=1)
    wo_copy.wait()

    for start in range(0, D_MODEL, 1024):
        value = jnp.dot(mixed, wo_buf[:, start:start + 1024], preferred_element_type=F32)
        part_ref[:, :, start:start + 1024] = value.reshape(16, 8, 1024).astype(BF16)

    def end_out(head, carry):
        out_copy(k_buf, nk, ko_sem, head).wait()
        out_copy(v_buf, nv, vo_sem, head).wait()
        return carry
    lax.fori_loop(0, HEADS, end_out, 0)


def self_stage(x_in, tok_row, rel_t, norm_row, w_q, w_k, w_v, w_o, sk_t, sv_t):
    hbm = pl.BlockSpec(memory_space=pltpu.HBM)
    vmem = pl.BlockSpec(memory_space=pltpu.VMEM)
    cache = jax.ShapeDtypeStruct((T_LEN, HEADS, HEAD_DIM, ROWS), BF16)
    dma = pltpu.SemaphoreType.DMA
    return pl.pallas_call(
        self_kernel,
        out_shape=(jax.ShapeDtypeStruct((16, 8, D_MODEL), BF16), cache, cache),
        in_specs=[hbm, vmem, vmem, vmem] + [hbm] * 6,
        out_specs=(vmem, hbm, hbm),
        scratch_shapes=[
            pltpu.VMEM((ROWS, D_MODEL), BF16), pltpu.VMEM((ROWS, D_MODEL), BF16),
            pltpu.VMEM((D_MODEL, 3 * FLAT), BF16), pltpu.VMEM((FLAT, D_MODEL), BF16),
            pltpu.VMEM((T_LEN, HEADS, HEAD_DIM, ROWS), BF16), pltpu.VMEM((T_LEN, HEADS, HEAD_DIM, ROWS), BF16),
            pltpu.VMEM((ROWS, 3 * FLAT), F32), pltpu.VMEM((FLAT, ROWS), F32),
            pltpu.VMEM((FLAT, ROWS), BF16), pltpu.VMEM((FLAT, ROWS), BF16),
            pltpu.VMEM((HEADS, T_LEN, ROWS), F32), pltpu.VMEM((HEADS, T_LEN, ROWS), F32), pltpu.VMEM((FLAT, ROWS), F32),
            pltpu.VMEM((1, D_MODEL), F32),
            dma, dma((N_CHUNK, 3)), dma, dma((HEADS,)), dma((HEADS,)), dma((HEADS,)), dma((HEADS,)),
        ],
        compiler_params=pltpu.CompilerParams(vmem_limit_bytes=60 * 1024 * 1024),
        cost_estimate=pl.CostEstimate(flops=10 ** 9, bytes_accessed=50 * 2 ** 20, transcendentals=0),
        name='self_stage',
    )(x_in, tok_row, rel_t, norm_row, w_q, w_k, w_v, w_o, sk_t, sv_t)


GROUPS = 2
GROUP_ROWS = ROWS // GROUPS
OWN = GROUP_ROWS // 8
STEP_ROWS = 16
SPLIT = 2
BUNDLE = 2
OUT_COLS = D_MODEL // SPLIT
STEPS = ROWS // STEP_ROWS
GROUP_STEPS = STEPS // GROUPS
SLOTS = 4
PAIR = 2 * HEADS
MESH = pl.DeviceIdType.MESH


def layer_kernel(part_hbm, x_hbm, enc_ref, nc_ref, nm_ref, ck, cv, wcq, wco, wg, wu, wd,
                 out_hbm,
                 x_own, g_buf, u_buf, d_buf, co_buf, k_buf, v_buf, part, d2d_buf, chip_sum, rs_buf, h_full,
                 h_rows, resid, q_buf, mixed, hidden, mask_buf, norm_rows,
                 p_sem, o_sem, x_sem, cq_sem, co_sem, g_sem, u_sem, d_sem, k_sem, v_sem,
                 dd_send, dd_recv, rs_send, rs_recv, ag_send, ag_recv, fw_send, fw_recv):
    me = lax.axis_index('tp')
    core = me % 2
    chip = me // 2
    partner = me + 1 - 2 * core
    chips = (chip + 1 - 2 * (chip % 2), (chip + 2) % 4, 3 - chip)
    peers = tuple(other * 2 + core for other in chips)

    barrier = pltpu.get_barrier_semaphore()
    for dev in (partner,) + peers:
        pl.semaphore_signal(barrier, inc=1, device_id={'tp': dev}, device_id_type=MESH)

    def block(group, half, which):
        return group * 8 + half * 4 + which

    x_copies = [pltpu.make_async_copy(x_hbm.at[block(g, core, chip)], x_own.at[g], x_sem.at[g]) for g in range(GROUPS)]
    cq_copy = pltpu.make_async_copy(wcq, g_buf.at[:, pl.ds(0, FLAT)], cq_sem)
    co_copy = pltpu.make_async_copy(wco, co_buf, co_sem)
    g_copy = pltpu.make_async_copy(wg, g_buf, g_sem)
    u_copy = pltpu.make_async_copy(wu, u_buf, u_sem)
    d_copy = pltpu.make_async_copy(wd, d_buf, d_sem)
    step_len = STEP_ROWS * FLAT

    def kv_copies(step):
        slot = step % SLOTS
        span = pl.ds(pl.multiple_of(step * step_len, step_len), step_len)
        return (pltpu.make_async_copy(ck.at[span, :], k_buf.at[slot], k_sem.at[slot]),
                pltpu.make_async_copy(cv.at[span, :], v_buf.at[slot], v_sem.at[slot]))

    def kv_start(step, carry=0):
        for copy in kv_copies(step):
            copy.start()
        return carry

    part_copies = [pltpu.make_async_copy(part_hbm.at[pl.ds(g * 8, 8)], part.at[pl.ds(g * 8, 8)], p_sem.at[g]) for g in range(GROUPS)]
    out_copies = [pltpu.make_async_copy(h_full.at[pl.ds(g * 8, 8)], out_hbm.at[pl.ds(g * 8, 8)], o_sem.at[g]) for g in range(GROUPS)]
    for copy in part_copies + x_copies:
        copy.start()
    cq_copy.start()
    lax.fori_loop(0, SLOTS, kv_start, 0)
    co_copy.start()
    u_copy.start()
    d_copy.start()

    norm_rows[0] = lane_row(nc_ref[...])
    norm_rows[1] = lane_row(nm_ref[...])
    mask_buf[...] = jnp.where(enc_ref[...] != 0, 0.0, NEG_FILL)
    pl.semaphore_wait(barrier, 4)

    def columns(part_no):
        return pl.ds(part_no * OUT_COLS, OUT_COLS)

    def d2d(group, src, part_no):
        return pltpu.make_async_remote_copy(
            src_ref=src.at[pl.ds(block(group, 1 - core, 0), 4), :, columns(part_no)],
            dst_ref=d2d_buf.at[group, :, :, columns(part_no)],
            send_sem=dd_send.at[group, part_no], recv_sem=dd_recv.at[group, part_no],
            device_id={'tp': partner}, device_id_type=MESH)

    def scatter(group, j, part_no):
        return pltpu.make_async_remote_copy(
            src_ref=chip_sum.at[group, chips[j], :, columns(part_no)], dst_ref=rs_buf.at[group, j, :, columns(part_no)],
            send_sem=rs_send.at[group, j, part_no], recv_sem=rs_recv.at[group, j, part_no],
            device_id={'tp': peers[j]}, device_id_type=MESH)

    def gather(group, j, part_no):
        piece = h_full.at[block(group, core, chip), :, columns(part_no)]
        return pltpu.make_async_remote_copy(
            src_ref=piece, dst_ref=piece, send_sem=ag_send.at[group, j, part_no], recv_sem=ag_recv.at[group, j, part_no],
            device_id={'tp': peers[j]}, device_id_type=MESH)

    def forward(group, j, part_no):
        piece = h_full.at[block(group, core, chip if j == 3 else chips[j]), :, columns(part_no)]
        return pltpu.make_async_remote_copy(
            src_ref=piece, dst_ref=piece, send_sem=fw_send.at[group, j, part_no], recv_sem=fw_recv.at[group, j, part_no],
            device_id={'tp': partner}, device_id_type=MESH)

    def d2d_start(group, src):
        for part_no in range(SPLIT):
            d2d(group, src, part_no).start()

    def reduce_chip(group, src):
        for part_no in range(SPLIT):
            d2d(group, src, part_no).wait()
            cols = columns(part_no)
            for which in range(4):
                total = src[block(group, core, which), :, cols].astype(F32) + d2d_buf[group, which, :, cols].astype(F32)
                chip_sum[group, which, :, cols] = total.astype(BF16)
            for j in (2, 0, 1):
                scatter(group, j, part_no).start()

    def send_rows(group, part_no):
        for j in (2, 0, 1):
            gather(group, j, part_no).start()
        forward(group, 3, part_no).start()

    def finish_rows(group, norm, last):
        own = block(group, core, chip)
        for part_no in range(SPLIT):
            cols = columns(part_no)
            total = resid[group, :, cols] + chip_sum[group, chip, :, cols].astype(F32)
            for j in range(3):
                scatter(group, j, part_no).wait()
                total = total + rs_buf[group, j, :, cols].astype(F32)
            if last:
                h_full[own, :, cols] = total.astype(BF16)
                send_rows(group, part_no)
            else:
                resid[group, :, cols] = total
        if not last:
            h_full[own] = rms_norm(resid[group], norm_rows[norm])
            for part_no in range(SPLIT):
                send_rows(group, part_no)

    def pass_on(group):
        for part_no in range(SPLIT):
            for j in (0, 1, 2):
                gather(group, j, part_no).wait()
                forward(group, j, part_no).start()

    def rows_ready(group):
        for part_no in range(SPLIT):
            for j in (3, 0, 1, 2):
                forward(group, j, part_no).wait()

    def collect(group):
        rows_ready(group)

        def two(i, carry):
            pair = h_full[pl.ds(group * 8 + i * 2, 2)].astype(F32).reshape(16, D_MODEL)
            h_rows[pl.ds(pl.multiple_of(group * GROUP_ROWS + i * 16, 16), 16), :] = pair.astype(BF16)
            return carry
        lax.fori_loop(0, GROUP_ROWS // 16, two, 0)

    def out_product(group, left, weight_ref):
        rows = left()
        for part_no in range(SPLIT):
            cols = slice(part_no * OUT_COLS, (part_no + 1) * OUT_COLS)
            value = jnp.dot(rows, weight_ref[:, cols], preferred_element_type=F32)
            part[group * 8:(group + 1) * 8, :, cols] = value.reshape(8, OWN, OUT_COLS).astype(BF16)
            d2d(group, part, part_no).start()

    own_head = (lax.broadcasted_iota(jnp.int32, (HEADS, FLAT), 1) // HEAD_DIM
                == lax.broadcasted_iota(jnp.int32, (HEADS, FLAT), 0))

    def queries(group):
        span = slice(group * GROUP_ROWS, (group + 1) * GROUP_ROWS)
        value = jnp.dot(h_rows[span, :], g_buf[:, :FLAT], preferred_element_type=F32)
        q_buf[span, :] = value.astype(BF16).astype(F32)

    def cross_step(step):
        slot = step % SLOTS
        for copy in kv_copies(step):
            copy.wait()
        base = pl.multiple_of(step * STEP_ROWS, STEP_ROWS)
        q_rows = q_buf[pl.ds(base, STEP_ROWS), :]
        mask_rows = mask_buf[pl.ds(base, STEP_ROWS), :]
        zeros = jnp.zeros((HEADS, S_LEN), F32)
        bundles = [range(first, first + BUNDLE) for first in range(0, STEP_ROWS // 2, BUNDLE)]

        def two(buf, pair):
            return jnp.concatenate([buf[slot, (2 * pair + i) * FLAT:(2 * pair + i + 1) * FLAT, :] for i in range(2)], axis=1)

        all_scores = []
        for pairs in bundles:
            scores = []
            for pair in pairs:
                left = jnp.concatenate([jnp.where(own_head, q_rows[2 * pair + i:2 * pair + i + 1, :], 0.0) for i in range(2)], axis=0)
                both = jnp.dot(left.astype(BF16), two(k_buf, pair), preferred_element_type=F32)
                scores.append(both[:HEADS, :S_LEN] + mask_rows[2 * pair:2 * pair + 1, :])
                scores.append(both[HEADS:, S_LEN:] + mask_rows[2 * pair + 1:2 * pair + 2, :])
            all_scores.append(jnp.concatenate(scores, axis=0))
        rows = []
        for pairs, score in zip(bundles, all_scores):
            weight = jnp.exp(score - jnp.max(score, axis=1, keepdims=True))
            weight = weight / jnp.sum(weight, axis=1, keepdims=True)
            for k, pair in enumerate(pairs):
                first = weight[2 * k * HEADS:(2 * k + 1) * HEADS, :]
                second = weight[(2 * k + 1) * HEADS:(2 * k + 2) * HEADS, :]
                left = jnp.concatenate([jnp.concatenate([first, zeros], axis=1), jnp.concatenate([zeros, second], axis=1)], axis=0)
                both = lax.dot_general(left.astype(BF16), two(v_buf, pair), (((1,), (1,)), ((), ())), preferred_element_type=F32)
                for i in range(2):
                    mine = jnp.where(own_head, both[i * HEADS:(i + 1) * HEADS, :], 0.0)
                    rows.append(jnp.sum(mine, axis=0, keepdims=True))
        mixed[pl.ds(base, STEP_ROWS), :] = jnp.concatenate(rows, axis=0)

    def cross_out(group):
        span = slice(group * GROUP_ROWS, (group + 1) * GROUP_ROWS)
        out_product(group, lambda: mixed[span, :].astype(BF16), co_buf)

    def mlp_in(group, at_block):
        span = slice(group * GROUP_ROWS, (group + 1) * GROUP_ROWS)

        for i in range(UNITS // 256):
            at_block(i)
            cols = slice(i * 256, (i + 1) * 256)
            gate = jnp.dot(h_rows[span, :], g_buf[:, cols], preferred_element_type=F32)
            up = jnp.dot(h_rows[span, :], u_buf[:, cols], preferred_element_type=F32)
            hidden[:, cols] = (jax.nn.gelu(gate, approximate=True) * up).astype(BF16)

    def mlp_out(group):
        out_product(group, lambda: hidden[...], d_buf)

    for g in range(GROUPS):
        part_copies[g].wait()
        d2d_start(g, part)
    for g in range(GROUPS):
        reduce_chip(g, part)
    for g in range(GROUPS):
        x_copies[g].wait()
        resid[g] = x_own[g].astype(F32)
        finish_rows(g, 0, False)
    pass_on(0)
    cq_copy.wait()
    collect(0)
    queries(0)

    def first_group(i, carry):
        cross_step(i)
        kv_start(i + SLOTS)
        return carry
    lax.fori_loop(0, GROUP_STEPS - 1, first_group, 0)
    pass_on(1)
    first_group(GROUP_STEPS - 1, 0)
    co_copy.wait()
    cross_out(0)
    collect(1)
    queries(1)
    g_copy.start()
    reduce_chip(0, part)

    def second_group(i, carry):
        cross_step(i + GROUP_STEPS)
        return carry
    lax.fori_loop(0, GROUP_STEPS, second_group, 0)
    cross_out(1)
    finish_rows(0, 1, False)
    reduce_chip(1, part)
    pass_on(0)
    finish_rows(1, 1, False)
    collect(0)
    g_copy.wait()
    u_copy.wait()
    d_copy.wait()

    mlp_in(0, lambda i: None)
    pass_on(1)
    mlp_out(0)
    collect(1)
    mlp_in(1, lambda i: reduce_chip(0, part) if i == 1 else None)
    finish_rows(0, 1, True)
    mlp_out(1)
    reduce_chip(1, part)
    pass_on(0)
    finish_rows(1, 1, True)
    rows_ready(0)
    out_copies[0].start()
    pass_on(1)
    rows_ready(1)
    out_copies[1].start()
    for copy in out_copies:
        copy.wait()


def layer_stage(part, x_blocks, enc_mask, norm_cross, norm_mlp, ck, cv, cross_q, cross_o, w_gate, w_up, w_down):
    hbm = pl.BlockSpec(memory_space=pltpu.HBM)
    vmem = pl.BlockSpec(memory_space=pltpu.VMEM)
    dma = pltpu.SemaphoreType.DMA
    blocks = (2 * 8, OWN, D_MODEL)
    return pl.pallas_call(
        layer_kernel,
        out_shape=jax.ShapeDtypeStruct(blocks, BF16),
        in_specs=[hbm, hbm, vmem, vmem, vmem] + [hbm] * 7,
        out_specs=hbm,
        scratch_shapes=[
            pltpu.VMEM((GROUPS, OWN, D_MODEL), BF16),
            pltpu.VMEM((D_MODEL, UNITS), BF16), pltpu.VMEM((D_MODEL, UNITS), BF16), pltpu.VMEM((UNITS, D_MODEL), BF16),
            pltpu.VMEM((FLAT, D_MODEL), BF16),
            pltpu.VMEM((SLOTS, STEP_ROWS * FLAT, S_LEN), BF16), pltpu.VMEM((SLOTS, STEP_ROWS * FLAT, S_LEN), BF16),
            pltpu.VMEM(blocks, BF16),
            pltpu.VMEM((GROUPS, 4, OWN, D_MODEL), BF16), pltpu.VMEM((GROUPS, 4, OWN, D_MODEL), BF16),
            pltpu.VMEM((GROUPS, 3, OWN, D_MODEL), BF16), pltpu.VMEM(blocks, BF16),
            pltpu.VMEM((ROWS, D_MODEL), BF16), pltpu.VMEM((GROUPS, OWN, D_MODEL), F32),
            pltpu.VMEM((ROWS, FLAT), F32), pltpu.VMEM((ROWS, FLAT), F32), pltpu.VMEM((GROUP_ROWS, UNITS), BF16),
            pltpu.VMEM((ROWS, S_LEN), F32), pltpu.VMEM((2, 1, D_MODEL), F32),
            dma((GROUPS,)), dma((GROUPS,)), dma((GROUPS,)), dma, dma, dma, dma, dma, dma((SLOTS,)), dma((SLOTS,)),
            dma((GROUPS, SPLIT)), dma((GROUPS, SPLIT)), dma((GROUPS, 3, SPLIT)), dma((GROUPS, 3, SPLIT)),
            dma((GROUPS, 3, SPLIT)), dma((GROUPS, 3, SPLIT)),
            dma((GROUPS, 4, SPLIT)), dma((GROUPS, 4, SPLIT)),
        ],
        compiler_params=pltpu.CompilerParams(collective_id=0, has_side_effects=True, vmem_limit_bytes=59 * 1024 * 1024),
        cost_estimate=pl.CostEstimate(flops=10 ** 10, bytes_accessed=70 * 2 ** 20, transcendentals=0),
        name='layer_stage',
    )(part, x_blocks, enc_mask, norm_cross, norm_mlp, ck, cv, cross_q, cross_o, w_gate, w_up, w_down)


def solution(mesh):
    def local_layer(x_in, tok_pos, self_k, self_v, cross_k, cross_v, enc_mask, rel_bias, w_q, w_k, w_v, w_o, cross_q, cross_o, w_gate, w_up, w_down, norm_self, norm_cross, norm_mlp):
        part, new_k, new_v = self_stage(
            x_in, tok_pos.reshape(1, ROWS), rel_bias.T, norm_self.reshape(32, 128), w_q, w_k, w_v, w_o,
            jnp.transpose(self_k, (1, 2, 3, 0)), jnp.transpose(self_v, (1, 2, 3, 0)))
        new_self_k = jnp.transpose(new_k, (3, 0, 1, 2))
        new_self_v = jnp.transpose(new_v, (3, 0, 1, 2))
        ck = jnp.transpose(cross_k, (0, 2, 3, 1)).reshape(ROWS * FLAT, S_LEN)
        cv = jnp.transpose(cross_v, (0, 2, 3, 1)).reshape(ROWS * FLAT, S_LEN)
        out = layer_stage(part, x_in.reshape(2 * 8, OWN, D_MODEL), enc_mask, norm_cross.reshape(32, 128),
                          norm_mlp.reshape(32, 128), ck, cv, cross_q, cross_o, w_gate, w_up, w_down)
        return out.reshape(ROWS, D_MODEL), new_self_k, new_self_v

    cache_spec = P('dp', None, 'tp', None)
    split_cols = P(None, 'tp')
    split_rows = P('tp', None)
    in_specs = (P('dp', None), P('dp'), cache_spec, cache_spec, cache_spec, cache_spec, P('dp', None), P(None, 'tp'), split_cols, split_cols, split_cols, split_rows, split_cols, split_rows, split_cols, split_cols, split_rows, P(None), P(None), P(None))
    out_specs = (P('dp', None), cache_spec, cache_spec)
    return jax.shard_map(local_layer, mesh=mesh, in_specs=in_specs, out_specs=out_specs, check_vma=False)
```

```python
import math
import jax
import jax.numpy as jnp
import numpy as np
from jax import lax
from jax.experimental import pallas as pl
from jax.experimental.pallas import tpu as pltpu
from jax.sharding import PartitionSpec as P

F32 = jnp.float32
BF16 = jnp.bfloat16
BUCKET_EDGES = tuple(int(math.ceil(16.0 * 8.0 ** (bucket_step / 16.0))) for bucket_step in range(1, 16))
NEG_FILL = -1e30
ROWS, T_LEN, S_LEN, HEADS, HEAD_DIM = 128, 64, 128, 8, 64
D_MODEL, FLAT, UNITS = 4096, 512, 1280
K_CHUNK = 1024
N_CHUNK = D_MODEL // K_CHUNK


def rms_norm(values, norm_scale):
    inv_rms = lax.rsqrt(jnp.mean(values * values, axis=-1, keepdims=True) + 1e-6)
    return (values * inv_rms * norm_scale).astype(BF16)


def lane_row(blocks):
    rows = blocks.astype(F32)
    return jnp.concatenate([rows[i:i + 1, :] for i in range(rows.shape[0])], axis=1)


def bias_table(rel_bias_t, tok_row):
    step = lax.broadcasted_iota(jnp.int32, (T_LEN, 32), 0)
    bucket = lax.broadcasted_iota(jnp.int32, (T_LEN, 32), 1)
    distance = (T_LEN - 1) - step
    far = jnp.full_like(distance, 16)
    for edge in BUCKET_EDGES:
        far = far + (distance >= edge).astype(jnp.int32)
    own_bucket = jnp.where(distance < 16, distance, far)
    one_hot = (bucket == own_bucket).astype(F32)
    by_step = lax.dot_general(one_hot, rel_bias_t, (((1,), (1,)), ((), ())),
                              precision=lax.Precision.HIGHEST, preferred_element_type=F32)
    shift = (T_LEN - 1) - tok_row
    position = lax.broadcasted_iota(jnp.int32, (T_LEN, ROWS), 0)
    allowed = position <= tok_row
    tables = []
    for head in range(HEADS):
        table = jnp.broadcast_to(by_step[:, head:head + 1], (T_LEN, ROWS))
        for bit in (32, 16, 8, 4, 2, 1):
            moved = jnp.concatenate([table[bit:], table[:bit]], axis=0)
            table = jnp.where((shift & bit) != 0, moved, table)
        tables.append(jnp.where(allowed, table, NEG_FILL))
    return tables


def self_kernel(x_hbm, tok_hbm, rel_hbm, norm_hbm, wq, wk, wv, wo, sk, sv,
                part_hbm, nk, nv,
                x_buf, h_buf, w_buf, wo_buf, k_buf, v_buf, acc, q_t, kn_t, vn_t, bias, probs, mix, norm_row, part_ref,
                tok_ref, rel_ref, norm_ref, small_sem, part_sem, x_sem, w_sem, wo_sem, k_sem, v_sem, ko_sem, vo_sem):
    x_copy = pltpu.make_async_copy(x_hbm, x_buf, x_sem)
    x_copy.start()
    small_copies = [pltpu.make_async_copy(src, dst, small_sem.at[i]) for i, (src, dst) in enumerate(
        ((tok_hbm, tok_ref), (rel_hbm, rel_ref), (norm_hbm, norm_ref)))]
    for copy in small_copies:
        copy.start()
    srcs = (wq, wk, wv)

    def w_copy(chunk, which):
        rows = pl.ds(pl.multiple_of(chunk * K_CHUNK, K_CHUNK), K_CHUNK)
        return pltpu.make_async_copy(srcs[which].at[rows, :], w_buf.at[rows, pl.ds(which * FLAT, FLAT)],
                                     w_sem.at[chunk, which])

    def span(group):
        return pl.ds(pl.multiple_of(group * 8, 8), 8)

    def in_copy(src, buf, sem, group):
        return pltpu.make_async_copy(src.at[span(group)], buf.at[span(group)], sem.at[group])

    def out_copy(buf, dst, sem, group):
        return pltpu.make_async_copy(buf.at[span(group)], dst.at[span(group)], sem.at[group])

    for chunk in range(1):
        for which in range(3):
            w_copy(chunk, which).start()

    wo_copy = pltpu.make_async_copy(wo, wo_buf, wo_sem)

    for copy in small_copies:
        copy.wait()
    tok_row = tok_ref[...]
    for head, table in enumerate(bias_table(rel_ref[...], tok_row)):
        bias[head] = table

    norm_row[...] = lane_row(norm_ref[...])
    x_copy.wait()
    for chunk in range(1, N_CHUNK):
        for which in range(3):
            w_copy(chunk, which).start()

    def norm_rows(step, carry):
        rows = pl.ds(pl.multiple_of(step * 16, 16), 16)
        h_buf[rows, :] = rms_norm(x_buf[rows, :].astype(F32), norm_row[...])
        return carry
    lax.fori_loop(0, ROWS // 16, norm_rows, 0)

    acc[...] = jnp.zeros_like(acc)

    def qkv_step(chunk, carry):
        for which in range(3):
            w_copy(chunk, which).wait()
            rows = pl.ds(pl.multiple_of(chunk * K_CHUNK, K_CHUNK), K_CHUNK)
            cols = slice(which * FLAT, (which + 1) * FLAT)
            acc[:, cols] += jnp.dot(h_buf[:, rows], w_buf[rows, cols], preferred_element_type=F32)

        @pl.when(chunk == 0)
        def _():
            for src, buf, sem in ((sk, k_buf, k_sem), (sv, v_buf, v_sem)):
                for group in range(T_LEN // 8):
                    in_copy(src, buf, sem, group).start()
            wo_copy.start()
        return carry
    lax.fori_loop(0, N_CHUNK, qkv_step, 0)

    for which, dst in enumerate((q_t, kn_t, vn_t)):
        for block in range(FLAT // 128):
            start = which * FLAT + block * 128
            turned = jnp.transpose(acc[:, start:start + 128])
            dst[block * 128:(block + 1) * 128, :] = turned.astype(BF16).astype(dst.dtype)

    tok_b = jnp.broadcast_to(tok_row.astype(F32), (HEAD_DIM, ROWS)).astype(BF16)

    def score_group(group, carry):
        in_copy(sk, k_buf, k_sem, group).wait()
        at_tok = tok_b - (group * 8).astype(F32).astype(BF16)

        def per_head(head, inner):
            lanes = pl.ds(pl.multiple_of(head * HEAD_DIM, HEAD_DIM), HEAD_DIM)
            query = q_t[lanes, :]
            fresh_k = kn_t[lanes, :]
            rows = []
            for i in range(8):
                step = group * 8 + i
                keys = jnp.where(at_tok == jnp.asarray(i, BF16), fresh_k, k_buf[step, head])
                k_buf[step, head] = keys
                rows.append(jnp.sum(keys.astype(F32) * query, axis=0, keepdims=True))
            probs[head, span(group), :] = jnp.concatenate(rows, axis=0)
            return inner
        lax.fori_loop(0, HEADS, per_head, 0, unroll=4)
        out_copy(k_buf, nk, ko_sem, group).start()
        return carry
    lax.fori_loop(0, T_LEN // 8, score_group, 0)

    def soften(head, carry):
        scores = probs[head] + bias[head]
        weights = jnp.exp(scores - jnp.max(scores, axis=0, keepdims=True))
        weights = weights / jnp.sum(weights, axis=0, keepdims=True)
        probs[head] = weights.astype(BF16).astype(F32)
        return carry
    lax.fori_loop(0, HEADS, soften, 0)
    mix[...] = jnp.zeros_like(mix)

    def mix_group(group, carry):
        in_copy(sv, v_buf, v_sem, group).wait()
        at_tok = tok_b - (group * 8).astype(F32).astype(BF16)

        def per_head(head, inner):
            lanes = pl.ds(pl.multiple_of(head * HEAD_DIM, HEAD_DIM), HEAD_DIM)
            fresh_v = vn_t[lanes, :]
            total = mix[lanes, :]
            for i in range(8):
                step = group * 8 + i
                vals = jnp.where(at_tok == jnp.asarray(i, BF16), fresh_v, v_buf[step, head])
                v_buf[step, head] = vals
                total = total + vals.astype(F32) * probs[head, pl.ds(step, 1), :]
            mix[lanes, :] = total
            return inner
        lax.fori_loop(0, HEADS, per_head, 0, unroll=4)
        out_copy(v_buf, nv, vo_sem, group).start()
        return carry
    lax.fori_loop(0, T_LEN // 8, mix_group, 0)

    mixed = jnp.concatenate([jnp.transpose(mix[block * 128:(block + 1) * 128, :]).astype(BF16)
                             for block in range(FLAT // 128)], axis=1)
    wo_copy.wait()

    def part_copy(part_no):
        cols = pl.ds(part_no * 1024, 1024)
        return pltpu.make_async_copy(part_ref.at[:, :, cols], part_hbm.at[:, :, cols], part_sem.at[part_no])

    for start in range(0, D_MODEL, 1024):
        value = jnp.dot(mixed, wo_buf[:, start:start + 1024], preferred_element_type=F32)
        part_ref[:, :, start:start + 1024] = value.reshape(16, 8, 1024).astype(BF16)
        part_copy(start // 1024).start()

    for part_no in range(4):
        part_copy(part_no).wait()

    def end_out(head, carry):
        out_copy(k_buf, nk, ko_sem, head).wait()
        out_copy(v_buf, nv, vo_sem, head).wait()
        return carry
    lax.fori_loop(0, HEADS, end_out, 0)


def self_stage(x_in, tok_row, rel_t, norm_row, w_q, w_k, w_v, w_o, sk_t, sv_t):
    hbm = pl.BlockSpec(memory_space=pltpu.HBM)
    cache = jax.ShapeDtypeStruct((T_LEN, HEADS, HEAD_DIM, ROWS), BF16)
    dma = pltpu.SemaphoreType.DMA
    return pl.pallas_call(
        self_kernel,
        out_shape=(jax.ShapeDtypeStruct((16, 8, D_MODEL), BF16), cache, cache),
        in_specs=[hbm] * 10,
        out_specs=(hbm, hbm, hbm),
        scratch_shapes=[
            pltpu.VMEM((ROWS, D_MODEL), BF16), pltpu.VMEM((ROWS, D_MODEL), BF16),
            pltpu.VMEM((D_MODEL, 3 * FLAT), BF16), pltpu.VMEM((FLAT, D_MODEL), BF16),
            pltpu.VMEM((T_LEN, HEADS, HEAD_DIM, ROWS), BF16), pltpu.VMEM((T_LEN, HEADS, HEAD_DIM, ROWS), BF16),
            pltpu.VMEM((ROWS, 3 * FLAT), F32), pltpu.VMEM((FLAT, ROWS), F32),
            pltpu.VMEM((FLAT, ROWS), BF16), pltpu.VMEM((FLAT, ROWS), BF16),
            pltpu.VMEM((HEADS, T_LEN, ROWS), F32), pltpu.VMEM((HEADS, T_LEN, ROWS), F32), pltpu.VMEM((FLAT, ROWS), F32),
            pltpu.VMEM((1, D_MODEL), F32), pltpu.VMEM((16, 8, D_MODEL), BF16),
            pltpu.VMEM((1, ROWS), jnp.int32), pltpu.VMEM((HEADS, 32), F32), pltpu.VMEM((32, 128), BF16), dma((3,)),
            dma((4,)), dma, dma((N_CHUNK, 3)), dma, dma((HEADS,)), dma((HEADS,)), dma((HEADS,)), dma((HEADS,)),
        ],
        compiler_params=pltpu.CompilerParams(vmem_limit_bytes=60 * 1024 * 1024),
        cost_estimate=pl.CostEstimate(flops=10 ** 9, bytes_accessed=50 * 2 ** 20, transcendentals=0),
        name='self_stage',
    )(x_in, tok_row, rel_t, norm_row, w_q, w_k, w_v, w_o, sk_t, sv_t)


GROUPS = 2
GROUP_ROWS = ROWS // GROUPS
OWN = GROUP_ROWS // 8
STEP_ROWS = 16
SPLIT = 2
BUNDLE = 2
OUT_COLS = D_MODEL // SPLIT
STEPS = ROWS // STEP_ROWS
GROUP_STEPS = STEPS // GROUPS
SLOTS = 4
PAIR = 2 * HEADS
MESH = pl.DeviceIdType.MESH


def layer_kernel(part_hbm, x_hbm, enc_hbm, nc_hbm, nm_hbm, ck, cv, wcq, wco, wg, wu, wd,
                 out_hbm,
                 x_own, g_buf, u_buf, d_buf, co_buf, k_buf, v_buf, part, d2d_buf, chip_sum, rs_buf, h_full,
                 h_rows, resid, q_buf, mixed, hidden, mask_buf, norm_rows,
                 enc_ref, nc_ref, nm_ref, small_sem, p_sem, o_sem, x_sem, cq_sem, co_sem, g_sem, u_sem, d_sem, k_sem, v_sem,
                 dd_send, dd_recv, rs_send, rs_recv, ag_send, ag_recv, fw_send, fw_recv):
    me = lax.axis_index('tp')
    core = me % 2
    chip = me // 2
    partner = me + 1 - 2 * core
    chips = (chip + 1 - 2 * (chip % 2), (chip + 2) % 4, 3 - chip)
    peers = tuple(other * 2 + core for other in chips)

    barrier = pltpu.get_barrier_semaphore()
    for dev in (partner,) + peers:
        pl.semaphore_signal(barrier, inc=1, device_id={'tp': dev}, device_id_type=MESH)

    def block(group, half, which):
        return group * 8 + half * 4 + which

    x_copies = [pltpu.make_async_copy(x_hbm.at[block(g, core, chip)], x_own.at[g], x_sem.at[g]) for g in range(GROUPS)]
    cq_copy = pltpu.make_async_copy(wcq, g_buf.at[:, pl.ds(0, FLAT)], cq_sem)
    co_copy = pltpu.make_async_copy(wco, co_buf, co_sem)
    g_copy = pltpu.make_async_copy(wg, g_buf, g_sem)
    u_copy = pltpu.make_async_copy(wu, u_buf, u_sem)
    d_copy = pltpu.make_async_copy(wd, d_buf, d_sem)
    step_len = STEP_ROWS * FLAT

    def kv_copies(step):
        slot = step % SLOTS
        span = pl.ds(pl.multiple_of(step * step_len, step_len), step_len)
        return (pltpu.make_async_copy(ck.at[span, :], k_buf.at[slot], k_sem.at[slot]),
                pltpu.make_async_copy(cv.at[span, :], v_buf.at[slot], v_sem.at[slot]))

    def kv_start(step, carry=0):
        for copy in kv_copies(step):
            copy.start()
        return carry

    part_copies = [pltpu.make_async_copy(part_hbm.at[pl.ds(g * 8, 8)], part.at[pl.ds(g * 8, 8)], p_sem.at[g]) for g in range(GROUPS)]
    out_copies = [pltpu.make_async_copy(h_full.at[pl.ds(g * 8, 8)], out_hbm.at[pl.ds(g * 8, 8)], o_sem.at[g]) for g in range(GROUPS)]
    small_copies = [pltpu.make_async_copy(src, dst, small_sem.at[i]) for i, (src, dst) in enumerate(
        ((enc_hbm, enc_ref), (nc_hbm, nc_ref), (nm_hbm, nm_ref)))]
    for copy in part_copies + x_copies + small_copies:
        copy.start()
    cq_copy.start()
    lax.fori_loop(0, SLOTS, kv_start, 0)
    co_copy.start()
    u_copy.start()
    d_copy.start()

    pl.semaphore_wait(barrier, 4)

    def columns(part_no):
        return pl.ds(part_no * OUT_COLS, OUT_COLS)

    def d2d(group, src, part_no):
        return pltpu.make_async_remote_copy(
            src_ref=src.at[pl.ds(block(group, 1 - core, 0), 4), :, columns(part_no)],
            dst_ref=d2d_buf.at[group, :, :, columns(part_no)],
            send_sem=dd_send.at[group, part_no], recv_sem=dd_recv.at[group, part_no],
            device_id={'tp': partner}, device_id_type=MESH)

    def scatter(group, j, part_no):
        return pltpu.make_async_remote_copy(
            src_ref=chip_sum.at[group, chips[j], :, columns(part_no)], dst_ref=rs_buf.at[group, j, :, columns(part_no)],
            send_sem=rs_send.at[group, j, part_no], recv_sem=rs_recv.at[group, j, part_no],
            device_id={'tp': peers[j]}, device_id_type=MESH)

    def gather(group, j, part_no):
        piece = h_full.at[block(group, core, chip), :, columns(part_no)]
        return pltpu.make_async_remote_copy(
            src_ref=piece, dst_ref=piece, send_sem=ag_send.at[group, j, part_no], recv_sem=ag_recv.at[group, j, part_no],
            device_id={'tp': peers[j]}, device_id_type=MESH)

    def forward(group, j, part_no):
        piece = h_full.at[block(group, core, chip if j == 3 else chips[j]), :, columns(part_no)]
        return pltpu.make_async_remote_copy(
            src_ref=piece, dst_ref=piece, send_sem=fw_send.at[group, j, part_no], recv_sem=fw_recv.at[group, j, part_no],
            device_id={'tp': partner}, device_id_type=MESH)

    def d2d_start(group, src):
        for part_no in range(SPLIT):
            d2d(group, src, part_no).start()

    def reduce_chip(group, src):
        for part_no in range(SPLIT):
            d2d(group, src, part_no).wait()
            cols = columns(part_no)
            for which in range(4):
                total = src[block(group, core, which), :, cols].astype(F32) + d2d_buf[group, which, :, cols].astype(F32)
                chip_sum[group, which, :, cols] = total.astype(BF16)
            for j in (2, 0, 1):
                scatter(group, j, part_no).start()

    def send_rows(group, part_no):
        for j in (2, 0, 1):
            gather(group, j, part_no).start()
        forward(group, 3, part_no).start()

    def finish_rows(group, norm, last):
        own = block(group, core, chip)
        for part_no in range(SPLIT):
            cols = columns(part_no)
            total = resid[group, :, cols] + chip_sum[group, chip, :, cols].astype(F32)
            for j in range(3):
                scatter(group, j, part_no).wait()
                total = total + rs_buf[group, j, :, cols].astype(F32)
            if last:
                h_full[own, :, cols] = total.astype(BF16)
                send_rows(group, part_no)
            else:
                resid[group, :, cols] = total
        if not last:
            h_full[own] = rms_norm(resid[group], norm_rows[norm])
            for part_no in range(SPLIT):
                send_rows(group, part_no)

    def pass_on(group):
        for part_no in range(SPLIT):
            for j in (0, 1, 2):
                gather(group, j, part_no).wait()
                forward(group, j, part_no).start()

    def rows_ready(group):
        for part_no in range(SPLIT):
            for j in (3, 0, 1, 2):
                forward(group, j, part_no).wait()

    def collect(group):
        rows_ready(group)

        def two(i, carry):
            pair = h_full[pl.ds(group * 8 + i * 2, 2)].astype(F32).reshape(16, D_MODEL)
            h_rows[pl.ds(pl.multiple_of(group * GROUP_ROWS + i * 16, 16), 16), :] = pair.astype(BF16)
            return carry
        lax.fori_loop(0, GROUP_ROWS // 16, two, 0)

    def out_product(group, left, weight_ref):
        rows = left()
        for part_no in range(SPLIT):
            cols = slice(part_no * OUT_COLS, (part_no + 1) * OUT_COLS)
            value = jnp.dot(rows, weight_ref[:, cols], preferred_element_type=F32)
            part[group * 8:(group + 1) * 8, :, cols] = value.reshape(8, OWN, OUT_COLS).astype(BF16)
            d2d(group, part, part_no).start()

    own_head = (lax.broadcasted_iota(jnp.int32, (HEADS, FLAT), 1) // HEAD_DIM
                == lax.broadcasted_iota(jnp.int32, (HEADS, FLAT), 0))

    def queries(group):
        span = slice(group * GROUP_ROWS, (group + 1) * GROUP_ROWS)
        value = jnp.dot(h_rows[span, :], g_buf[:, :FLAT], preferred_element_type=F32)
        q_buf[span, :] = value.astype(BF16).astype(F32)

    def cross_step(step):
        slot = step % SLOTS
        for copy in kv_copies(step):
            copy.wait()
        base = pl.multiple_of(step * STEP_ROWS, STEP_ROWS)
        q_rows = q_buf[pl.ds(base, STEP_ROWS), :]
        mask_rows = mask_buf[pl.ds(base, STEP_ROWS), :]
        zeros = jnp.zeros((HEADS, S_LEN), F32)
        bundles = [range(first, first + BUNDLE) for first in range(0, STEP_ROWS // 2, BUNDLE)]

        def two(buf, pair):
            return jnp.concatenate([buf[slot, (2 * pair + i) * FLAT:(2 * pair + i + 1) * FLAT, :] for i in range(2)], axis=1)

        all_scores = []
        for pairs in bundles:
            scores = []
            for pair in pairs:
                left = jnp.concatenate([jnp.where(own_head, q_rows[2 * pair + i:2 * pair + i + 1, :], 0.0) for i in range(2)], axis=0)
                both = jnp.dot(left.astype(BF16), two(k_buf, pair), preferred_element_type=F32)
                scores.append(both[:HEADS, :S_LEN] + mask_rows[2 * pair:2 * pair + 1, :])
                scores.append(both[HEADS:, S_LEN:] + mask_rows[2 * pair + 1:2 * pair + 2, :])
            all_scores.append(jnp.concatenate(scores, axis=0))
        rows = []
        for pairs, score in zip(bundles, all_scores):
            weight = jnp.exp(score - jnp.max(score, axis=1, keepdims=True))
            weight = weight / jnp.sum(weight, axis=1, keepdims=True)
            for k, pair in enumerate(pairs):
                first = weight[2 * k * HEADS:(2 * k + 1) * HEADS, :]
                second = weight[(2 * k + 1) * HEADS:(2 * k + 2) * HEADS, :]
                left = jnp.concatenate([jnp.concatenate([first, zeros], axis=1), jnp.concatenate([zeros, second], axis=1)], axis=0)
                both = lax.dot_general(left.astype(BF16), two(v_buf, pair), (((1,), (1,)), ((), ())), preferred_element_type=F32)
                for i in range(2):
                    mine = jnp.where(own_head, both[i * HEADS:(i + 1) * HEADS, :], 0.0)
                    rows.append(jnp.sum(mine, axis=0, keepdims=True))
        mixed[pl.ds(base, STEP_ROWS), :] = jnp.concatenate(rows, axis=0)

    def cross_out(group):
        span = slice(group * GROUP_ROWS, (group + 1) * GROUP_ROWS)
        out_product(group, lambda: mixed[span, :].astype(BF16), co_buf)

    def mlp_in(group, at_block):
        span = slice(group * GROUP_ROWS, (group + 1) * GROUP_ROWS)

        for i in range(UNITS // 256):
            at_block(i)
            cols = slice(i * 256, (i + 1) * 256)
            gate = jnp.dot(h_rows[span, :], g_buf[:, cols], preferred_element_type=F32)
            up = jnp.dot(h_rows[span, :], u_buf[:, cols], preferred_element_type=F32)
            hidden[:, cols] = (jax.nn.gelu(gate, approximate=True) * up).astype(BF16)

    def mlp_out(group):
        out_product(group, lambda: hidden[...], d_buf)

    for g in range(GROUPS):
        part_copies[g].wait()
        d2d_start(g, part)
    for copy in small_copies:
        copy.wait()
    norm_rows[0] = lane_row(nc_ref[...])
    norm_rows[1] = lane_row(nm_ref[...])
    mask_buf[...] = jnp.where(enc_ref[...] != 0, 0.0, NEG_FILL)
    for g in range(GROUPS):
        reduce_chip(g, part)
    for g in range(GROUPS):
        x_copies[g].wait()
        resid[g] = x_own[g].astype(F32)
        finish_rows(g, 0, False)
    pass_on(0)
    cq_copy.wait()
    collect(0)
    queries(0)

    def first_group(i, carry):
        cross_step(i)
        kv_start(i + SLOTS)
        return carry
    lax.fori_loop(0, GROUP_STEPS - 1, first_group, 0)
    pass_on(1)
    first_group(GROUP_STEPS - 1, 0)
    co_copy.wait()
    cross_out(0)
    collect(1)
    queries(1)
    g_copy.start()
    reduce_chip(0, part)

    def second_group(i, carry):
        cross_step(i + GROUP_STEPS)
        return carry
    lax.fori_loop(0, GROUP_STEPS, second_group, 0)
    cross_out(1)
    finish_rows(0, 1, False)
    reduce_chip(1, part)
    pass_on(0)
    finish_rows(1, 1, False)
    collect(0)
    g_copy.wait()
    u_copy.wait()
    d_copy.wait()

    mlp_in(0, lambda i: None)
    pass_on(1)
    mlp_out(0)
    collect(1)
    mlp_in(1, lambda i: reduce_chip(0, part) if i == 1 else None)
    finish_rows(0, 1, True)
    mlp_out(1)
    reduce_chip(1, part)
    pass_on(0)
    finish_rows(1, 1, True)
    rows_ready(0)
    out_copies[0].start()
    pass_on(1)
    rows_ready(1)
    out_copies[1].start()
    for copy in out_copies:
        copy.wait()


def layer_stage(part, x_blocks, enc_mask, norm_cross, norm_mlp, ck, cv, cross_q, cross_o, w_gate, w_up, w_down):
    hbm = pl.BlockSpec(memory_space=pltpu.HBM)
    dma = pltpu.SemaphoreType.DMA
    blocks = (2 * 8, OWN, D_MODEL)
    return pl.pallas_call(
        layer_kernel,
        out_shape=jax.ShapeDtypeStruct(blocks, BF16),
        in_specs=[hbm] * 12,
        out_specs=hbm,
        scratch_shapes=[
            pltpu.VMEM((GROUPS, OWN, D_MODEL), BF16),
            pltpu.VMEM((D_MODEL, UNITS), BF16), pltpu.VMEM((D_MODEL, UNITS), BF16), pltpu.VMEM((UNITS, D_MODEL), BF16),
            pltpu.VMEM((FLAT, D_MODEL), BF16),
            pltpu.VMEM((SLOTS, STEP_ROWS * FLAT, S_LEN), BF16), pltpu.VMEM((SLOTS, STEP_ROWS * FLAT, S_LEN), BF16),
            pltpu.VMEM(blocks, BF16),
            pltpu.VMEM((GROUPS, 4, OWN, D_MODEL), BF16), pltpu.VMEM((GROUPS, 4, OWN, D_MODEL), BF16),
            pltpu.VMEM((GROUPS, 3, OWN, D_MODEL), BF16), pltpu.VMEM(blocks, BF16),
            pltpu.VMEM((ROWS, D_MODEL), BF16), pltpu.VMEM((GROUPS, OWN, D_MODEL), F32),
            pltpu.VMEM((ROWS, FLAT), F32), pltpu.VMEM((ROWS, FLAT), F32), pltpu.VMEM((GROUP_ROWS, UNITS), BF16),
            pltpu.VMEM((ROWS, S_LEN), F32), pltpu.VMEM((2, 1, D_MODEL), F32),
            pltpu.VMEM((ROWS, S_LEN), jnp.int32), pltpu.VMEM((32, 128), BF16), pltpu.VMEM((32, 128), BF16), dma((3,)),
            dma((GROUPS,)), dma((GROUPS,)), dma((GROUPS,)), dma, dma, dma, dma, dma, dma((SLOTS,)), dma((SLOTS,)),
            dma((GROUPS, SPLIT)), dma((GROUPS, SPLIT)), dma((GROUPS, 3, SPLIT)), dma((GROUPS, 3, SPLIT)),
            dma((GROUPS, 3, SPLIT)), dma((GROUPS, 3, SPLIT)),
            dma((GROUPS, 4, SPLIT)), dma((GROUPS, 4, SPLIT)),
        ],
        compiler_params=pltpu.CompilerParams(collective_id=0, has_side_effects=True, vmem_limit_bytes=59 * 1024 * 1024),
        cost_estimate=pl.CostEstimate(flops=10 ** 10, bytes_accessed=70 * 2 ** 20, transcendentals=0),
        name='layer_stage',
    )(part, x_blocks, enc_mask, norm_cross, norm_mlp, ck, cv, cross_q, cross_o, w_gate, w_up, w_down)


def solution(mesh):
    def local_layer(x_in, tok_pos, self_k, self_v, cross_k, cross_v, enc_mask, rel_bias, w_q, w_k, w_v, w_o, cross_q, cross_o, w_gate, w_up, w_down, norm_self, norm_cross, norm_mlp):
        part, new_k, new_v = self_stage(
            x_in, tok_pos.reshape(1, ROWS), rel_bias.T, norm_self.reshape(32, 128), w_q, w_k, w_v, w_o,
            jnp.transpose(self_k, (1, 2, 3, 0)), jnp.transpose(self_v, (1, 2, 3, 0)))
        new_self_k = jnp.transpose(new_k, (3, 0, 1, 2))
        new_self_v = jnp.transpose(new_v, (3, 0, 1, 2))
        ck = jnp.transpose(cross_k, (0, 2, 3, 1)).reshape(ROWS * FLAT, S_LEN)
        cv = jnp.transpose(cross_v, (0, 2, 3, 1)).reshape(ROWS * FLAT, S_LEN)
        out = layer_stage(part, x_in.reshape(2 * 8, OWN, D_MODEL), enc_mask, norm_cross.reshape(32, 128),
                          norm_mlp.reshape(32, 128), ck, cv, cross_q, cross_o, w_gate, w_up, w_down)
        return out.reshape(ROWS, D_MODEL), new_self_k, new_self_v

    cache_spec = P('dp', None, 'tp', None)
    split_cols = P(None, 'tp')
    split_rows = P('tp', None)
    in_specs = (P('dp', None), P('dp'), cache_spec, cache_spec, cache_spec, cache_spec, P('dp', None), P(None, 'tp'), split_cols, split_cols, split_cols, split_rows, split_cols, split_rows, split_cols, split_cols, split_rows, P(None), P(None), P(None))
    out_specs = (P('dp', None), cache_spec, cache_spec)
    return jax.shard_map(local_layer, mesh=mesh, in_specs=in_specs, out_specs=out_specs, check_vma=False)
```

```python
import math
import jax
import jax.numpy as jnp
import numpy as np
from jax import lax
from jax.experimental import pallas as pl
from jax.experimental.pallas import tpu as pltpu
from jax.sharding import PartitionSpec as P

F32 = jnp.float32
BF16 = jnp.bfloat16
BUCKET_EDGES = tuple(int(math.ceil(16.0 * 8.0 ** (bucket_step / 16.0))) for bucket_step in range(1, 16))
NEG_FILL = -1e30
ROWS, T_LEN, S_LEN, HEADS, HEAD_DIM = 128, 64, 128, 8, 64
D_MODEL, FLAT, UNITS = 4096, 512, 1280
K_CHUNK = 1024
N_CHUNK = D_MODEL // K_CHUNK


def rms_norm(values, norm_scale):
    inv_rms = lax.rsqrt(jnp.mean(values * values, axis=-1, keepdims=True) + 1e-6)
    return (values * inv_rms * norm_scale).astype(BF16)


def lane_row(blocks):
    rows = blocks.astype(F32)
    return jnp.concatenate([rows[i:i + 1, :] for i in range(rows.shape[0])], axis=1)


def bias_table(rel_bias_t, tok_row):
    step = lax.broadcasted_iota(jnp.int32, (T_LEN, 32), 0)
    bucket = lax.broadcasted_iota(jnp.int32, (T_LEN, 32), 1)
    distance = (T_LEN - 1) - step
    far = jnp.full_like(distance, 16)
    for edge in BUCKET_EDGES:
        far = far + (distance >= edge).astype(jnp.int32)
    own_bucket = jnp.where(distance < 16, distance, far)
    one_hot = (bucket == own_bucket).astype(F32)
    by_step = lax.dot_general(one_hot, rel_bias_t, (((1,), (1,)), ((), ())),
                              precision=lax.Precision.HIGHEST, preferred_element_type=F32)
    shift = (T_LEN - 1) - tok_row
    position = lax.broadcasted_iota(jnp.int32, (T_LEN, ROWS), 0)
    allowed = position <= tok_row
    tables = []
    for head in range(HEADS):
        table = jnp.broadcast_to(by_step[:, head:head + 1], (T_LEN, ROWS))
        for bit in (32, 16, 8, 4, 2, 1):
            moved = jnp.concatenate([table[bit:], table[:bit]], axis=0)
            table = jnp.where((shift & bit) != 0, moved, table)
        tables.append(jnp.where(allowed, table, NEG_FILL))
    return tables


def self_kernel(x_hbm, tok_hbm, rel_hbm, norm_hbm, wq, wk, wv, wo, sk, sv,
                part_hbm, nk, nv,
                x_buf, h_buf, w_buf, wo_buf, k_buf, v_buf, acc, q_t, kn_t, vn_t, bias, probs, mix, norm_row, part_ref,
                tok_ref, rel_ref, norm_ref, small_sem, part_sem, x_sem, w_sem, wo_sem, k_sem, v_sem, ko_sem, vo_sem):
    x_copy = pltpu.make_async_copy(x_hbm, x_buf, x_sem)
    x_copy.start()
    small_copies = [pltpu.make_async_copy(src, dst, small_sem.at[i]) for i, (src, dst) in enumerate(
        ((tok_hbm, tok_ref), (rel_hbm, rel_ref), (norm_hbm, norm_ref)))]
    for copy in small_copies:
        copy.start()
    srcs = (wq, wk, wv)

    def w_copy(chunk, which):
        rows = pl.ds(pl.multiple_of(chunk * K_CHUNK, K_CHUNK), K_CHUNK)
        return pltpu.make_async_copy(srcs[which].at[rows, :], w_buf.at[rows, pl.ds(which * FLAT, FLAT)],
                                     w_sem.at[chunk, which])

    def span(group):
        return pl.ds(pl.multiple_of(group * 8, 8), 8)

    def in_copy(src, buf, sem, group):
        return pltpu.make_async_copy(src.at[span(group)], buf.at[span(group)], sem.at[group])

    def out_copy(buf, dst, sem, group):
        return pltpu.make_async_copy(buf.at[span(group)], dst.at[span(group)], sem.at[group])

    for chunk in range(2):
        for which in range(3):
            w_copy(chunk, which).start()

    wo_copy = pltpu.make_async_copy(wo, wo_buf, wo_sem)

    for copy in small_copies:
        copy.wait()
    tok_row = tok_ref[...]
    for head, table in enumerate(bias_table(rel_ref[...], tok_row)):
        bias[head] = table

    norm_row[...] = lane_row(norm_ref[...])
    x_copy.wait()
    for chunk in range(2, N_CHUNK):
        for which in range(3):
            w_copy(chunk, which).start()

    def norm_rows(step, carry):
        rows = pl.ds(pl.multiple_of(step * 16, 16), 16)
        h_buf[rows, :] = rms_norm(x_buf[rows, :].astype(F32), norm_row[...])
        return carry
    lax.fori_loop(0, ROWS // 16, norm_rows, 0)

    acc[...] = jnp.zeros_like(acc)

    def qkv_step(chunk, carry):
        for which in range(3):
            w_copy(chunk, which).wait()
            rows = pl.ds(pl.multiple_of(chunk * K_CHUNK, K_CHUNK), K_CHUNK)
            cols = slice(which * FLAT, (which + 1) * FLAT)
            acc[:, cols] += jnp.dot(h_buf[:, rows], w_buf[rows, cols], preferred_element_type=F32)

        @pl.when(chunk == 0)
        def _():
            for src, buf, sem in ((sk, k_buf, k_sem), (sv, v_buf, v_sem)):
                for group in range(T_LEN // 8):
                    in_copy(src, buf, sem, group).start()
            wo_copy.start()
        return carry
    lax.fori_loop(0, N_CHUNK, qkv_step, 0)

    for which, dst in enumerate((q_t, kn_t, vn_t)):
        for block in range(FLAT // 128):
            start = which * FLAT + block * 128
            turned = jnp.transpose(acc[:, start:start + 128])
            dst[block * 128:(block + 1) * 128, :] = turned.astype(BF16).astype(dst.dtype)

    tok_b = jnp.broadcast_to(tok_row.astype(F32), (HEAD_DIM, ROWS)).astype(BF16)

    def score_group(group, carry):
        in_copy(sk, k_buf, k_sem, group).wait()
        at_tok = tok_b - (group * 8).astype(F32).astype(BF16)

        def per_head(head, inner):
            lanes = pl.ds(pl.multiple_of(head * HEAD_DIM, HEAD_DIM), HEAD_DIM)
            query = q_t[lanes, :]
            fresh_k = kn_t[lanes, :]
            rows = []
            for i in range(8):
                step = group * 8 + i
                keys = jnp.where(at_tok == jnp.asarray(i, BF16), fresh_k, k_buf[step, head])
                k_buf[step, head] = keys
                rows.append(jnp.sum(keys.astype(F32) * query, axis=0, keepdims=True))
            probs[head, span(group), :] = jnp.concatenate(rows, axis=0)
            return inner
        lax.fori_loop(0, HEADS, per_head, 0, unroll=4)
        out_copy(k_buf, nk, ko_sem, group).start()
        return carry
    lax.fori_loop(0, T_LEN // 8, score_group, 0)

    def soften(head, carry):
        scores = probs[head] + bias[head]
        weights = jnp.exp(scores - jnp.max(scores, axis=0, keepdims=True))
        weights = weights / jnp.sum(weights, axis=0, keepdims=True)
        probs[head] = weights.astype(BF16).astype(F32)
        return carry
    lax.fori_loop(0, HEADS, soften, 0, unroll=8)
    mix[...] = jnp.zeros_like(mix)

    def mix_group(group, carry):
        in_copy(sv, v_buf, v_sem, group).wait()
        at_tok = tok_b - (group * 8).astype(F32).astype(BF16)

        def per_head(head, inner):
            lanes = pl.ds(pl.multiple_of(head * HEAD_DIM, HEAD_DIM), HEAD_DIM)
            fresh_v = vn_t[lanes, :]
            total = mix[lanes, :]
            for i in range(8):
                step = group * 8 + i
                vals = jnp.where(at_tok == jnp.asarray(i, BF16), fresh_v, v_buf[step, head])
                v_buf[step, head] = vals
                total = total + vals.astype(F32) * probs[head, pl.ds(step, 1), :]
            mix[lanes, :] = total
            return inner
        lax.fori_loop(0, HEADS, per_head, 0, unroll=4)
        out_copy(v_buf, nv, vo_sem, group).start()
        return carry
    lax.fori_loop(0, T_LEN // 8, mix_group, 0)

    mixed = jnp.concatenate([jnp.transpose(mix[block * 128:(block + 1) * 128, :]).astype(BF16)
                             for block in range(FLAT // 128)], axis=1)
    wo_copy.wait()

    def part_copy(part_no):
        cols = pl.ds(part_no * 1024, 1024)
        return pltpu.make_async_copy(part_ref.at[:, :, cols], part_hbm.at[:, :, cols], part_sem.at[part_no])

    for start in range(0, D_MODEL, 1024):
        value = jnp.dot(mixed, wo_buf[:, start:start + 1024], preferred_element_type=F32)
        part_ref[:, :, start:start + 1024] = value.reshape(16, 8, 1024).astype(BF16)
        part_copy(start // 1024).start()

    for part_no in range(4):
        part_copy(part_no).wait()

    def end_out(head, carry):
        out_copy(k_buf, nk, ko_sem, head).wait()
        out_copy(v_buf, nv, vo_sem, head).wait()
        return carry
    lax.fori_loop(0, HEADS, end_out, 0)


def self_stage(x_in, tok_row, rel_t, norm_row, w_q, w_k, w_v, w_o, sk_t, sv_t):
    hbm = pl.BlockSpec(memory_space=pltpu.HBM)
    cache = jax.ShapeDtypeStruct((T_LEN, HEADS, HEAD_DIM, ROWS), BF16)
    dma = pltpu.SemaphoreType.DMA
    return pl.pallas_call(
        self_kernel,
        out_shape=(jax.ShapeDtypeStruct((16, 8, D_MODEL), BF16), cache, cache),
        in_specs=[hbm] * 10,
        out_specs=(hbm, hbm, hbm),
        scratch_shapes=[
            pltpu.VMEM((ROWS, D_MODEL), BF16), pltpu.VMEM((ROWS, D_MODEL), BF16),
            pltpu.VMEM((D_MODEL, 3 * FLAT), BF16), pltpu.VMEM((FLAT, D_MODEL), BF16),
            pltpu.VMEM((T_LEN, HEADS, HEAD_DIM, ROWS), BF16), pltpu.VMEM((T_LEN, HEADS, HEAD_DIM, ROWS), BF16),
            pltpu.VMEM((ROWS, 3 * FLAT), F32), pltpu.VMEM((FLAT, ROWS), F32),
            pltpu.VMEM((FLAT, ROWS), BF16), pltpu.VMEM((FLAT, ROWS), BF16),
            pltpu.VMEM((HEADS, T_LEN, ROWS), F32), pltpu.VMEM((HEADS, T_LEN, ROWS), F32), pltpu.VMEM((FLAT, ROWS), F32),
            pltpu.VMEM((1, D_MODEL), F32), pltpu.VMEM((16, 8, D_MODEL), BF16),
            pltpu.VMEM((1, ROWS), jnp.int32), pltpu.VMEM((HEADS, 32), F32), pltpu.VMEM((32, 128), BF16), dma((3,)),
            dma((4,)), dma, dma((N_CHUNK, 3)), dma, dma((HEADS,)), dma((HEADS,)), dma((HEADS,)), dma((HEADS,)),
        ],
        compiler_params=pltpu.CompilerParams(vmem_limit_bytes=60 * 1024 * 1024),
        cost_estimate=pl.CostEstimate(flops=10 ** 9, bytes_accessed=50 * 2 ** 20, transcendentals=0),
        name='self_stage',
    )(x_in, tok_row, rel_t, norm_row, w_q, w_k, w_v, w_o, sk_t, sv_t)


GROUPS = 2
GROUP_ROWS = ROWS // GROUPS
OWN = GROUP_ROWS // 8
STEP_ROWS = 16
SPLIT = 2
BUNDLE = 2
OUT_COLS = D_MODEL // SPLIT
STEPS = ROWS // STEP_ROWS
GROUP_STEPS = STEPS // GROUPS
SLOTS = 4
PAIR = 2 * HEADS
MESH = pl.DeviceIdType.MESH


def layer_kernel(part_hbm, x_hbm, enc_hbm, nc_hbm, nm_hbm, ck, cv, wcq, wco, wg, wu, wd,
                 out_hbm,
                 x_own, g_buf, u_buf, d_buf, co_buf, k_buf, v_buf, part, d2d_buf, chip_sum, rs_buf, h_full,
                 h_rows, resid, q_buf, mixed, hidden, mask_buf, norm_rows,
                 enc_ref, nc_ref, nm_ref, small_sem, p_sem, o_sem, x_sem, cq_sem, co_sem, g_sem, u_sem, d_sem, k_sem, v_sem,
                 dd_send, dd_recv, rs_send, rs_recv, ag_send, ag_recv, fw_send, fw_recv):
    me = lax.axis_index('tp')
    core = me % 2
    chip = me // 2
    partner = me + 1 - 2 * core
    chips = (chip + 1 - 2 * (chip % 2), (chip + 2) % 4, 3 - chip)
    peers = tuple(other * 2 + core for other in chips)

    barrier = pltpu.get_barrier_semaphore()
    for dev in (partner,) + peers:
        pl.semaphore_signal(barrier, inc=1, device_id={'tp': dev}, device_id_type=MESH)

    def block(group, half, which):
        return group * 8 + half * 4 + which

    x_copies = [pltpu.make_async_copy(x_hbm.at[block(g, core, chip)], x_own.at[g], x_sem.at[g]) for g in range(GROUPS)]
    cq_copy = pltpu.make_async_copy(wcq, g_buf.at[:, pl.ds(0, FLAT)], cq_sem)
    co_copy = pltpu.make_async_copy(wco, co_buf, co_sem)
    g_copy = pltpu.make_async_copy(wg, g_buf, g_sem)
    u_copy = pltpu.make_async_copy(wu, u_buf, u_sem)
    d_copy = pltpu.make_async_copy(wd, d_buf, d_sem)
    step_len = STEP_ROWS * FLAT

    def kv_copies(step):
        slot = step % SLOTS
        span = pl.ds(pl.multiple_of(step * step_len, step_len), step_len)
        return (pltpu.make_async_copy(ck.at[span, :], k_buf.at[slot], k_sem.at[slot]),
                pltpu.make_async_copy(cv.at[span, :], v_buf.at[slot], v_sem.at[slot]))

    def kv_start(step, carry=0):
        for copy in kv_copies(step):
            copy.start()
        return carry

    part_copies = [pltpu.make_async_copy(part_hbm.at[pl.ds(g * 8, 8)], part.at[pl.ds(g * 8, 8)], p_sem.at[g]) for g in range(GROUPS)]
    out_copies = [pltpu.make_async_copy(h_full.at[pl.ds(g * 8, 8)], out_hbm.at[pl.ds(g * 8, 8)], o_sem.at[g]) for g in range(GROUPS)]
    small_copies = [pltpu.make_async_copy(src, dst, small_sem.at[i]) for i, (src, dst) in enumerate(
        ((enc_hbm, enc_ref), (nc_hbm, nc_ref), (nm_hbm, nm_ref)))]
    for copy in part_copies + x_copies + small_copies:
        copy.start()

    pl.semaphore_wait(barrier, 4)

    def columns(part_no):
        return pl.ds(part_no * OUT_COLS, OUT_COLS)

    def d2d(group, src, part_no):
        return pltpu.make_async_remote_copy(
            src_ref=src.at[pl.ds(block(group, 1 - core, 0), 4), :, columns(part_no)],
            dst_ref=d2d_buf.at[group, :, :, columns(part_no)],
            send_sem=dd_send.at[group, part_no], recv_sem=dd_recv.at[group, part_no],
            device_id={'tp': partner}, device_id_type=MESH)

    def scatter(group, j, part_no):
        return pltpu.make_async_remote_copy(
            src_ref=chip_sum.at[group, chips[j], :, columns(part_no)], dst_ref=rs_buf.at[group, j, :, columns(part_no)],
            send_sem=rs_send.at[group, j, part_no], recv_sem=rs_recv.at[group, j, part_no],
            device_id={'tp': peers[j]}, device_id_type=MESH)

    def gather(group, j, part_no):
        piece = h_full.at[block(group, core, chip), :, columns(part_no)]
        return pltpu.make_async_remote_copy(
            src_ref=piece, dst_ref=piece, send_sem=ag_send.at[group, j, part_no], recv_sem=ag_recv.at[group, j, part_no],
            device_id={'tp': peers[j]}, device_id_type=MESH)

    def forward(group, j, part_no):
        piece = h_full.at[block(group, core, chip if j == 3 else chips[j]), :, columns(part_no)]
        return pltpu.make_async_remote_copy(
            src_ref=piece, dst_ref=piece, send_sem=fw_send.at[group, j, part_no], recv_sem=fw_recv.at[group, j, part_no],
            device_id={'tp': partner}, device_id_type=MESH)

    def d2d_start(group, src):
        for part_no in range(SPLIT):
            d2d(group, src, part_no).start()

    def reduce_chip(group, src):
        for part_no in range(SPLIT):
            d2d(group, src, part_no).wait()
            cols = columns(part_no)
            for which in range(4):
                total = src[block(group, core, which), :, cols].astype(F32) + d2d_buf[group, which, :, cols].astype(F32)
                chip_sum[group, which, :, cols] = total.astype(BF16)
            for j in (2, 0, 1):
                scatter(group, j, part_no).start()

    def send_rows(group, part_no):
        for j in (2, 0, 1):
            gather(group, j, part_no).start()
        forward(group, 3, part_no).start()

    def finish_rows(group, norm, last):
        own = block(group, core, chip)
        for part_no in range(SPLIT):
            cols = columns(part_no)
            total = resid[group, :, cols] + chip_sum[group, chip, :, cols].astype(F32)
            for j in range(3):
                scatter(group, j, part_no).wait()
                total = total + rs_buf[group, j, :, cols].astype(F32)
            if last:
                h_full[own, :, cols] = total.astype(BF16)
                send_rows(group, part_no)
            else:
                resid[group, :, cols] = total
        if not last:
            h_full[own] = rms_norm(resid[group], norm_rows[norm])
            for part_no in range(SPLIT):
                send_rows(group, part_no)

    def pass_on(group):
        for part_no in range(SPLIT):
            for j in (0, 1, 2):
                gather(group, j, part_no).wait()
                forward(group, j, part_no).start()

    def rows_ready(group):
        for part_no in range(SPLIT):
            for j in (3, 0, 1, 2):
                forward(group, j, part_no).wait()

    def collect(group):
        rows_ready(group)

        def two(i, carry):
            pair = h_full[pl.ds(group * 8 + i * 2, 2)].astype(F32).reshape(16, D_MODEL)
            h_rows[pl.ds(pl.multiple_of(group * GROUP_ROWS + i * 16, 16), 16), :] = pair.astype(BF16)
            return carry
        lax.fori_loop(0, GROUP_ROWS // 16, two, 0)

    def out_product(group, left, weight_ref):
        rows = left()
        for part_no in range(SPLIT):
            cols = slice(part_no * OUT_COLS, (part_no + 1) * OUT_COLS)
            value = jnp.dot(rows, weight_ref[:, cols], preferred_element_type=F32)
            part[group * 8:(group + 1) * 8, :, cols] = value.reshape(8, OWN, OUT_COLS).astype(BF16)
            d2d(group, part, part_no).start()

    own_head = (lax.broadcasted_iota(jnp.int32, (HEADS, FLAT), 1) // HEAD_DIM
                == lax.broadcasted_iota(jnp.int32, (HEADS, FLAT), 0))

    def queries(group):
        span = slice(group * GROUP_ROWS, (group + 1) * GROUP_ROWS)
        value = jnp.dot(h_rows[span, :], g_buf[:, :FLAT], preferred_element_type=F32)
        q_buf[span, :] = value.astype(BF16).astype(F32)

    def cross_step(step):
        slot = step % SLOTS
        for copy in kv_copies(step):
            copy.wait()
        base = pl.multiple_of(step * STEP_ROWS, STEP_ROWS)
        q_rows = q_buf[pl.ds(base, STEP_ROWS), :]
        mask_rows = mask_buf[pl.ds(base, STEP_ROWS), :]
        zeros = jnp.zeros((HEADS, S_LEN), F32)
        bundles = [range(first, first + BUNDLE) for first in range(0, STEP_ROWS // 2, BUNDLE)]

        def two(buf, pair):
            return jnp.concatenate([buf[slot, (2 * pair + i) * FLAT:(2 * pair + i + 1) * FLAT, :] for i in range(2)], axis=1)

        all_scores = []
        for pairs in bundles:
            scores = []
            for pair in pairs:
                left = jnp.concatenate([jnp.where(own_head, q_rows[2 * pair + i:2 * pair + i + 1, :], 0.0) for i in range(2)], axis=0)
                both = jnp.dot(left.astype(BF16), two(k_buf, pair), preferred_element_type=F32)
                scores.append(both[:HEADS, :S_LEN] + mask_rows[2 * pair:2 * pair + 1, :])
                scores.append(both[HEADS:, S_LEN:] + mask_rows[2 * pair + 1:2 * pair + 2, :])
            all_scores.append(jnp.concatenate(scores, axis=0))
        rows = []
        for pairs, score in zip(bundles, all_scores):
            weight = jnp.exp(score - jnp.max(score, axis=1, keepdims=True))
            weight = weight / jnp.sum(weight, axis=1, keepdims=True)
            for k, pair in enumerate(pairs):
                first = weight[2 * k * HEADS:(2 * k + 1) * HEADS, :]
                second = weight[(2 * k + 1) * HEADS:(2 * k + 2) * HEADS, :]
                left = jnp.concatenate([jnp.concatenate([first, zeros], axis=1), jnp.concatenate([zeros, second], axis=1)], axis=0)
                both = lax.dot_general(left.astype(BF16), two(v_buf, pair), (((1,), (1,)), ((), ())), preferred_element_type=F32)
                for i in range(2):
                    mine = jnp.where(own_head, both[i * HEADS:(i + 1) * HEADS, :], 0.0)
                    rows.append(jnp.sum(mine, axis=0, keepdims=True))
        mixed[pl.ds(base, STEP_ROWS), :] = jnp.concatenate(rows, axis=0)

    def cross_out(group):
        span = slice(group * GROUP_ROWS, (group + 1) * GROUP_ROWS)
        out_product(group, lambda: mixed[span, :].astype(BF16), co_buf)

    def mlp_in(group, at_block):
        span = slice(group * GROUP_ROWS, (group + 1) * GROUP_ROWS)

        for i in range(UNITS // 256):
            at_block(i)
            cols = slice(i * 256, (i + 1) * 256)
            gate = jnp.dot(h_rows[span, :], g_buf[:, cols], preferred_element_type=F32)
            up = jnp.dot(h_rows[span, :], u_buf[:, cols], preferred_element_type=F32)
            hidden[:, cols] = (jax.nn.gelu(gate, approximate=True) * up).astype(BF16)

    def mlp_out(group):
        out_product(group, lambda: hidden[...], d_buf)

    for g in range(GROUPS):
        part_copies[g].wait()
        d2d_start(g, part)
    cq_copy.start()
    lax.fori_loop(0, SLOTS, kv_start, 0)
    co_copy.start()
    u_copy.start()
    d_copy.start()
    for copy in small_copies:
        copy.wait()
    norm_rows[0] = lane_row(nc_ref[...])
    norm_rows[1] = lane_row(nm_ref[...])
    mask_buf[...] = jnp.where(enc_ref[...] != 0, 0.0, NEG_FILL)
    for g in range(GROUPS):
        reduce_chip(g, part)
    for g in range(GROUPS):
        x_copies[g].wait()
        resid[g] = x_own[g].astype(F32)
        finish_rows(g, 0, False)
    pass_on(0)
    cq_copy.wait()
    collect(0)
    queries(0)

    def first_group(i, carry):
        cross_step(i)
        kv_start(i + SLOTS)
        return carry
    lax.fori_loop(0, GROUP_STEPS - 1, first_group, 0)
    first_group(GROUP_STEPS - 1, 0)
    pass_on(1)
    co_copy.wait()
    cross_out(0)
    collect(1)
    queries(1)
    g_copy.start()
    reduce_chip(0, part)

    def second_group(i, carry):
        cross_step(i + GROUP_STEPS)
        return carry
    lax.fori_loop(0, GROUP_STEPS, second_group, 0)
    cross_out(1)
    finish_rows(0, 1, False)
    reduce_chip(1, part)
    pass_on(0)
    finish_rows(1, 1, False)
    collect(0)
    g_copy.wait()
    u_copy.wait()
    d_copy.wait()

    mlp_in(0, lambda i: None)
    pass_on(1)
    mlp_out(0)
    collect(1)
    mlp_in(1, lambda i: reduce_chip(0, part) if i == 1 else None)
    finish_rows(0, 1, True)
    mlp_out(1)
    reduce_chip(1, part)
    pass_on(0)
    finish_rows(1, 1, True)
    rows_ready(0)
    out_copies[0].start()
    pass_on(1)
    rows_ready(1)
    out_copies[1].start()
    for copy in out_copies:
        copy.wait()


def layer_stage(part, x_blocks, enc_mask, norm_cross, norm_mlp, ck, cv, cross_q, cross_o, w_gate, w_up, w_down):
    hbm = pl.BlockSpec(memory_space=pltpu.HBM)
    dma = pltpu.SemaphoreType.DMA
    blocks = (2 * 8, OWN, D_MODEL)
    return pl.pallas_call(
        layer_kernel,
        out_shape=jax.ShapeDtypeStruct(blocks, BF16),
        in_specs=[hbm] * 12,
        out_specs=hbm,
        scratch_shapes=[
            pltpu.VMEM((GROUPS, OWN, D_MODEL), BF16),
            pltpu.VMEM((D_MODEL, UNITS), BF16), pltpu.VMEM((D_MODEL, UNITS), BF16), pltpu.VMEM((UNITS, D_MODEL), BF16),
            pltpu.VMEM((FLAT, D_MODEL), BF16),
            pltpu.VMEM((SLOTS, STEP_ROWS * FLAT, S_LEN), BF16), pltpu.VMEM((SLOTS, STEP_ROWS * FLAT, S_LEN), BF16),
            pltpu.VMEM(blocks, BF16),
            pltpu.VMEM((GROUPS, 4, OWN, D_MODEL), BF16), pltpu.VMEM((GROUPS, 4, OWN, D_MODEL), BF16),
            pltpu.VMEM((GROUPS, 3, OWN, D_MODEL), BF16), pltpu.VMEM(blocks, BF16),
            pltpu.VMEM((ROWS, D_MODEL), BF16), pltpu.VMEM((GROUPS, OWN, D_MODEL), F32),
            pltpu.VMEM((ROWS, FLAT), F32), pltpu.VMEM((ROWS, FLAT), F32), pltpu.VMEM((GROUP_ROWS, UNITS), BF16),
            pltpu.VMEM((ROWS, S_LEN), F32), pltpu.VMEM((2, 1, D_MODEL), F32),
            pltpu.VMEM((ROWS, S_LEN), jnp.int32), pltpu.VMEM((32, 128), BF16), pltpu.VMEM((32, 128), BF16), dma((3,)),
            dma((GROUPS,)), dma((GROUPS,)), dma((GROUPS,)), dma, dma, dma, dma, dma, dma((SLOTS,)), dma((SLOTS,)),
            dma((GROUPS, SPLIT)), dma((GROUPS, SPLIT)), dma((GROUPS, 3, SPLIT)), dma((GROUPS, 3, SPLIT)),
            dma((GROUPS, 3, SPLIT)), dma((GROUPS, 3, SPLIT)),
            dma((GROUPS, 4, SPLIT)), dma((GROUPS, 4, SPLIT)),
        ],
        compiler_params=pltpu.CompilerParams(collective_id=0, has_side_effects=True, vmem_limit_bytes=59 * 1024 * 1024),
        cost_estimate=pl.CostEstimate(flops=10 ** 10, bytes_accessed=70 * 2 ** 20, transcendentals=0),
        name='layer_stage',
    )(part, x_blocks, enc_mask, norm_cross, norm_mlp, ck, cv, cross_q, cross_o, w_gate, w_up, w_down)


def solution(mesh):
    def local_layer(x_in, tok_pos, self_k, self_v, cross_k, cross_v, enc_mask, rel_bias, w_q, w_k, w_v, w_o, cross_q, cross_o, w_gate, w_up, w_down, norm_self, norm_cross, norm_mlp):
        part, new_k, new_v = self_stage(
            x_in, tok_pos.reshape(1, ROWS), rel_bias.T, norm_self.reshape(32, 128), w_q, w_k, w_v, w_o,
            jnp.transpose(self_k, (1, 2, 3, 0)), jnp.transpose(self_v, (1, 2, 3, 0)))
        new_self_k = jnp.transpose(new_k, (3, 0, 1, 2))
        new_self_v = jnp.transpose(new_v, (3, 0, 1, 2))
        ck = jnp.transpose(cross_k, (0, 2, 3, 1)).reshape(ROWS * FLAT, S_LEN)
        cv = jnp.transpose(cross_v, (0, 2, 3, 1)).reshape(ROWS * FLAT, S_LEN)
        out = layer_stage(part, x_in.reshape(2 * 8, OWN, D_MODEL), enc_mask, norm_cross.reshape(32, 128),
                          norm_mlp.reshape(32, 128), ck, cv, cross_q, cross_o, w_gate, w_up, w_down)
        return out.reshape(ROWS, D_MODEL), new_self_k, new_self_v

    cache_spec = P('dp', None, 'tp', None)
    split_cols = P(None, 'tp')
    split_rows = P('tp', None)
    in_specs = (P('dp', None), P('dp'), cache_spec, cache_spec, cache_spec, cache_spec, P('dp', None), P(None, 'tp'), split_cols, split_cols, split_cols, split_rows, split_cols, split_rows, split_cols, split_cols, split_rows, P(None), P(None), P(None))
    out_specs = (P('dp', None), cache_spec, cache_spec)
    return jax.shard_map(local_layer, mesh=mesh, in_specs=in_specs, out_specs=out_specs, check_vma=False)
```
